1024 devices in a mesh: gx: 32 (over y_hi, x), gy: 8 (over z), gz: 4 (over y_lo, core).
Axes of the slice: x: 8, y: 8 (y_hi: 4, y_lo: 2; y = y_hi * 2 + y_lo), z: 8, core: 2. Of those that a mesh axis runs over, the one named last changes fastest.
Arguments:
- displacement: float32 [32, 8, 18432], P('gx', 'gy', 'gz'), may hold values from -0.1 to 0.1
- species: int32 [32, 8, 6144], P('gx', 'gy', 'gz'), may hold values from 0 to 1
- centres: int32 [32, 8, 64], P('gx', 'gy', 'gz'), may hold values from 0 to 1535, as said below
- neighbours: int32 [32, 8, 2048], P('gx', 'gy', 'gz'), may hold values from 0 to 5183, as said below
- neighbour_count: int32 [32, 8, 64], P('gx', 'gy', 'gz'), may hold values from 1 to 32, as said below
- live_centres: int32 [32, 8, 4], P('gx', 'gy', 'gz'), may hold values from 8 to 16, as said below
- w_two: float32 [12, 64], replicated, may hold values from -1.75 to 1.75
- w_lat: float32 [64, 64], replicated, may hold values from -0.75 to 0.75
- w_env: float32 [64, 64], replicated, may hold values from -0.75 to 0.75
- w_out: float32 [256, 64], replicated, may hold values from -0.375 to 0.375
- readout: float32 [64], replicated, may hold values from -0.75 to 0.75
Outputs:
- centre_energy: float32 [32, 8, 64], P('gx', 'gy', 'gz')
- forces: float32 [32, 8, 18432], P('gx', 'gy', 'gz')
The draws below stay inside these ranges and needn't reach their ends.
Inputs may be any that keep to these rules, and one draw needn't show every extreme that they name: `centres`: local atom index of an owned atom; entries may repeat. `neighbours`: extended index of an atom whose cell lies within two cells of the centre's cell in each dimension, with squared cell distance at most 4; never the centre itself. `neighbour_count`: in every domain some centre has all 32 slots live. `live_centres`: some domain has all 16 centres live; the live centres are the first ones.
All inputs are finite; a program needn't handle non-finite values.
Results may differ from the reference program's by a relative error of at most 0.0003.
Values sent between devices are 32-bit elements; how exact they have to be, the bound alone decides.
No kernel may reach another device: no remote copies, remote signals or barrier semaphores. Data moves between devices by JAX's collectives and lax.ppermute only.
A program may use at most 32 MiB of HBM per device.

```python
import math
import jax
import jax.numpy as jnp
import numpy as np
from jax import lax

CELLS = 8
CENTRES = 16
NEIGH = 32
LATENT = 64
NBASIS = 8
SPECIES = 2
NX = 256
NY = 64
NZ = 32
N_GX = 32
N_GY = 8
N_GZ = 4


offset_rows = np.array([[0, 0, 0]] + [[a, b, c] for a in range(-2, 3) for b in range(-2, 3) for c in range(-2, 3) if 0 < a * a + b * b + c * c <= 4], np.int32)


def pair_lists(key):
    grid_x = NX // CELLS
    grid_y = NY // CELLS
    grid_z = NZ // CELLS
    extent = CELLS + 4
    base = jax.random.fold_in(key, 7)
    key_centre, key_offset, key_atom = jax.random.split(base, 3)
    centre = jax.random.randint(key_centre, (grid_x, grid_y, grid_z, CENTRES), 0, 3 * CELLS ** 3)
    atom_first = centre % 3
    cell_first = centre // 3
    loc_z = cell_first % CELLS
    loc_y = cell_first // CELLS % CELLS
    loc_x = cell_first // (CELLS * CELLS)
    choice_offset = jax.random.randint(key_offset, (grid_x, grid_y, grid_z, CENTRES, NEIGH), 0, offset_rows.shape[0])
    table = jnp.array(offset_rows)
    offsets = table[choice_offset]
    atom_second = jax.random.randint(key_atom, (grid_x, grid_y, grid_z, CENTRES, NEIGH), 0, 3)
    clash = (choice_offset == 0) & (atom_second == atom_first[..., None])
    atom_second = jnp.where(clash, (atom_first[..., None] + 1) % 3, atom_second)
    ext_x = loc_x[..., None] + 2 + offsets[..., 0]
    ext_y = loc_y[..., None] + 2 + offsets[..., 1]
    ext_z = loc_z[..., None] + 2 + offsets[..., 2]
    second = ((ext_x * extent + ext_y) * extent + ext_z) * 3 + atom_second
    return (centre.reshape(grid_x, grid_y, grid_z * CENTRES), second.reshape(grid_x, grid_y, grid_z * CENTRES * NEIGH))


def draw_centres(key, part):
    return pair_lists(key)[0].astype(jnp.int32)


def draw_neighbours(key, part):
    return pair_lists(key)[1].astype(jnp.int32)


def draw_neighbour_count(key, part):
    grid_x = NX // CELLS
    grid_y = NY // CELLS
    grid_z = NZ // CELLS
    key_level, key_count, key_pick = jax.random.split(jax.random.fold_in(key, 11), 3)
    level = jax.random.randint(key_level, (grid_x, grid_y, grid_z), 1, 5)
    ceiling = jnp.maximum(NEIGH * level // 4, 1)
    floor_count = jnp.maximum(ceiling // 2, 1)
    counts = jax.random.randint(key_count, (grid_x, grid_y, grid_z, CENTRES), floor_count[..., None], ceiling[..., None] + 1)
    pick = jax.random.randint(key_pick, (grid_x, grid_y, grid_z, 1), 0, CENTRES)
    ranks = jnp.arange(CENTRES, dtype=jnp.int32)
    counts = jnp.where(ranks == pick, NEIGH, counts)
    return counts.reshape(grid_x, grid_y, grid_z * CENTRES).astype(jnp.int32)


def draw_live_centres(key, part):
    grid_x = NX // CELLS
    grid_y = NY // CELLS
    grid_z = NZ // CELLS
    key_live, key_pick = jax.random.split(jax.random.fold_in(key, 13), 2)
    total = grid_x * grid_y * grid_z
    live = jax.random.randint(key_live, (total,), CENTRES // 2, CENTRES + 1)
    pick = jax.random.randint(key_pick, (), 0, total)
    live = jnp.where(jnp.arange(total, dtype=jnp.int32) == pick, CENTRES, live)
    return live.reshape(grid_x, grid_y, grid_z).astype(jnp.int32)


def set_ends(values, own_key, smallest, largest):
    spot = [jax.random.randint(jax.random.fold_in(own_key, axis), (), 0, length) for axis, length in enumerate(values.shape)]
    widest = values.shape.index(max(values.shape))
    neighbour = spot[:widest] + [(spot[widest] + 1) % values.shape[widest]] + spot[widest + 1:]
    return values.at[tuple(spot)].set(smallest).at[tuple(neighbour)].set(largest)


def shard_levels(key, shape, cuts, low, top_value):
    loudness, own = 1.0, jax.random.fold_in(key, 6)
    for axis_at, parts in cuts:
        draws = jnp.exp(jax.random.uniform(jax.random.fold_in(own, axis_at), (parts,), jnp.float32, low / len(cuts), top_value / len(cuts)))
        loudness = loudness * jnp.repeat(draws, shape[axis_at] // parts).reshape([-1 if axis == axis_at else 1 for axis in range(len(shape))])
    return loudness


def normal_values(stream_key, shape, spread, reach, kind=jnp.bfloat16):
    result = jax.random.normal(stream_key, shape, jnp.float32) * spread
    return jnp.minimum(jnp.maximum(result, -reach), reach).astype(kind)


def setup_inputs(seed: int = 0) -> dict:
    seeds = jax.random.split(jax.random.key(seed), 12)
    return {
        "displacement": jnp.clip(jax.random.uniform(seeds[0], (N_GX, N_GY, N_GZ * CELLS**3 * 9), jnp.float32, -0.1, 0.1) * shard_levels(seeds[0], (N_GX, N_GY, N_GZ * CELLS**3 * 9), ((0, 32), (1, 8), (2, 4)), -0.4, 0.0), -0.1, 0.1),
        "species": set_ends(jax.random.randint(seeds[1], (N_GX, N_GY, N_GZ * CELLS**3 * 3), 0, SPECIES), jax.random.fold_in(seeds[1], 1), 0, SPECIES - 1).astype(jnp.int32),
        "centres": draw_centres(jax.random.fold_in(seeds[11], 71), 0),
        "neighbours": draw_neighbours(jax.random.fold_in(seeds[11], 71), 0),
        "neighbour_count": draw_neighbour_count(jax.random.fold_in(seeds[11], 71), 0),
        "live_centres": draw_live_centres(jax.random.fold_in(seeds[11], 71), 0),
        "w_two": normal_values(seeds[6], (2 * SPECIES + NBASIS, LATENT), (2 * SPECIES + NBASIS) ** -0.5, 1.75, jnp.float32),
        "w_lat": normal_values(seeds[7], (LATENT, LATENT), LATENT ** -0.5, 0.75, jnp.float32),
        "w_env": normal_values(seeds[8], (LATENT, LATENT), LATENT ** -0.5, 0.75, jnp.float32),
        "w_out": normal_values(seeds[9], (4 * LATENT, LATENT), (4 * LATENT) ** -0.5, 0.375, jnp.float32),
        "readout": normal_values(seeds[10], (LATENT,), LATENT ** -0.5, 0.75, jnp.float32),
    }


cutoff = 6.0
cell_side = 3.1
env_scale = 0.2
site_rows = np.array([[0.25, 0.25, 0.25], [0.75, 0.75, 0.25], [0.25, 0.75, 0.75]], np.float32)

def mixing(weight, data):
    return jnp.dot(weight.T, data, precision=lax.Precision.HIGHEST, preferred_element_type=jnp.float32)

def harmonics(unit):
    ux, uy, uz = (unit[0], unit[1], unit[2])
    root3 = math.sqrt(3.0)
    root5 = math.sqrt(5.0)
    root15 = math.sqrt(15.0)
    return jnp.stack([jnp.ones_like(ux), root3 * ux, root3 * uy, root3 * uz, root15 * ux * uy, root15 * uy * uz, 0.5 * root5 * (3.0 * uz * uz - 1.0), root15 * ux * uz, 0.5 * root15 * (ux * ux - uy * uy)], 0)

def block_energy(rvec, kind_first, kind_second, live, w_two, w_lat, w_env, w_out, readout, slots):
    dist = jnp.sqrt(lax.optimization_barrier(jnp.sum(rvec * rvec, axis=0)))
    unit = rvec / dist
    ratio = dist / cutoff
    envelope = jnp.where(ratio < 1.0, 1.0 - 28.0 * ratio ** 6 + 48.0 * ratio ** 7 - 21.0 * ratio ** 8, 0.0)
    orders = jnp.arange(1, NBASIS + 1, dtype=jnp.float32)[:, None]
    basis = math.sqrt(2.0 / cutoff) * jnp.sin(orders * math.pi * dist[None, :] / cutoff) / dist[None, :] * envelope[None, :]
    kinds = jnp.arange(SPECIES, dtype=jnp.float32)[:, None]
    first_hot = (kind_first[None, :] == kinds).astype(jnp.float32)
    second_hot = (kind_second[None, :] == kinds).astype(jnp.float32)
    inputs = jnp.concatenate([first_hot, second_hot, basis], 0)
    hidden = jax.nn.silu(mixing(w_two, inputs))
    latent = jax.nn.silu(mixing(w_lat, hidden))
    weights = mixing(w_env, latent) * (envelope * live)[None, :]
    harm = harmonics(unit)
    width = latent.shape[0]
    centre_total = rvec.shape[1] // slots
    edge = (harm[:, None, :] * weights[None, :, :]).reshape(9, width, centre_total, slots)
    environ = env_scale * lax.optimization_barrier(jnp.sum(edge, axis=3))
    product = edge * environ[:, :, :, None]
    scalars = jnp.stack([product[0], lax.optimization_barrier(jnp.sum(product[1:4], axis=0)), lax.optimization_barrier(jnp.sum(product[4:9], axis=0))], 0)
    joined = jnp.concatenate([latent, scalars.reshape(3 * width, centre_total * slots)], 0)
    updated = jax.nn.silu(mixing(w_out, joined))
    pair_energy = jnp.dot(readout, updated, precision=lax.Precision.HIGHEST) * envelope * live
    return lax.optimization_barrier(jnp.sum(pair_energy.reshape(centre_total, slots), axis=1))

def to_grid(blocks, width):
    cube = blocks.reshape(N_GX, N_GY, N_GZ, CELLS, CELLS, CELLS, width)
    return jnp.transpose(cube, (0, 3, 1, 4, 2, 5, 6)).reshape(NX, NY, NZ, width)

def reference(displacement, species, centres, neighbours, neighbour_count, live_centres, w_two, w_lat, w_env, w_out, readout):
    side = CELLS
    extent = CELLS + 4
    domains = N_GX * N_GY * N_GZ
    shifts = to_grid(displacement, 9).reshape(NX, NY, NZ, 3, 3)
    kinds = to_grid(species, 3).astype(jnp.float32)
    centre_rows = centres.reshape(domains, CENTRES)
    neighbour_rows = neighbours.reshape(domains, CENTRES * NEIGH)
    count_rows = neighbour_count.reshape(domains, CENTRES)
    alive = live_centres.reshape(domains)
    sites = jnp.array(site_rows, dtype=jnp.float32)
    slot_ids = jnp.arange(NEIGH, dtype=jnp.int32)
    centre_ids = jnp.arange(CENTRES, dtype=jnp.int32)

    def one_domain(forces, index):
        dom_x = index // (N_GY * N_GZ)
        dom_y = index // N_GZ % N_GY
        dom_z = index % N_GZ
        first = jnp.repeat(centre_rows[index], NEIGH)
        atom_first = first % 3
        cell_first = first // 3
        loc_z = cell_first % side
        loc_y = cell_first // side % side
        loc_x = cell_first // (side * side)
        glob_xi = dom_x * side + loc_x
        glob_yi = dom_y * side + loc_y
        glob_zi = dom_z * side + loc_z
        second = neighbour_rows[index]
        atom_second = second % 3
        cell_second = second // 3
        ext_z = cell_second % extent - 2
        ext_y = cell_second // extent % extent - 2
        ext_x = cell_second // (extent * extent) - 2
        glob_xj = (dom_x * side + ext_x) % NX
        glob_yj = (dom_y * side + ext_y) % NY
        glob_zj = (dom_z * side + ext_z) % NZ
        place_first = jnp.stack([loc_x, loc_y, loc_z], 0).astype(jnp.float32) + sites[atom_first].T + shifts[glob_xi, glob_yi, glob_zi, atom_first].T
        place_second = jnp.stack([ext_x, ext_y, ext_z], 0).astype(jnp.float32) + sites[atom_second].T + shifts[glob_xj, glob_yj, glob_zj, atom_second].T
        rvec = (place_second - place_first) * cell_side
        kind_first = kinds[glob_xi, glob_yi, glob_zi, atom_first]
        kind_second = kinds[glob_xj, glob_yj, glob_zj, atom_second]
        live = ((slot_ids[None, :] < count_rows[index][:, None]) & (centre_ids[:, None] < alive[index])).reshape(-1).astype(jnp.float32)

        def energy_of(vectors):
            return block_energy(vectors, kind_first, kind_second, live, w_two, w_lat, w_env, w_out, readout, NEIGH)
        energy, pullback = jax.vjp(energy_of, rvec)
        grad = pullback(jnp.ones_like(energy))[0]
        index_first = ((glob_xi * NY + glob_yi) * NZ + glob_zi) * 3 + atom_first
        index_second = ((glob_xj * NY + glob_yj) * NZ + glob_zj) * 3 + atom_second
        forces = forces.at[index_second].add(-grad.T)
        forces = forces.at[index_first].add(grad.T)
        return (forces, energy)
    start = jnp.zeros((NX * NY * NZ * 3, 3), jnp.float32)
    forces, energies = lax.scan(one_domain, start, jnp.arange(domains, dtype=jnp.int32))
    grid = forces.reshape(N_GX, CELLS, N_GY, CELLS, N_GZ, CELLS, 9)
    blocks = jnp.transpose(grid, (0, 2, 4, 1, 3, 5, 6)).reshape(N_GX, N_GY, N_GZ * CELLS * CELLS * CELLS * 9)
    return (energies.reshape(N_GX, N_GY, N_GZ * CENTRES), blocks)
```

```python
import math

import jax
import jax.numpy as jnp
import numpy as np
from jax import lax
from jax.experimental import pallas as pl
from jax.experimental.pallas import tpu as pltpu
from jax.sharding import PartitionSpec as P

F32 = jnp.float32
BF16 = jnp.bfloat16
CELL = 3.1
CUT = 6.0
VM = pl.BlockSpec(memory_space=pltpu.VMEM)
SM = pl.BlockSpec(memory_space=pltpu.SMEM)
LANES = 144
PAIRS = 512
NS = 16


def call(kernel, outs, ins, name, scratch=(), flops=0):
    specs = [s for _, s in ins]
    return pl.pallas_call(
        kernel,
        out_shape=outs,
        in_specs=specs,
        out_specs=jax.tree.map(lambda _: VM, outs),
        scratch_shapes=list(scratch),
        name=name,
        cost_estimate=pl.CostEstimate(flops=flops, bytes_accessed=0, transcendentals=0),
    )(*[a for a, _ in ins])


def split(v, parts):
    out = []
    for _ in range(parts - 1):
        h = v.astype(BF16)
        out.append(h)
        v = v - h.astype(F32)
    out.append(v.astype(BF16))
    return out


def mm(a, b, dims=((1,), (0,))):
    return lax.dot_general(a, b, (dims, ((), ())), preferred_element_type=F32)


def pack_kernel(d_ref, s_ref, o_ref):
    for i in range(36):
        o_ref[i : i + 1, :] = d_ref[0, :, 128 * i : 128 * i + 128]
    for i in range(12):
        o_ref[36 + i : 37 + i, :] = s_ref[0, :, 128 * i : 128 * i + 128].astype(F32)


def zperm():
    m = np.zeros((3, 128, 256), np.float32)
    for s in range(12):
        d, z = (1, s + 6) if s < 2 else ((0, s - 2) if s < 10 else (2, s - 10))
        for a in range(3):
            for c in range(3):
                m[d, z * 9 + a * 3 + c, s * 12 + a * 4 + c] = 1.0
            m[d, 72 + z * 3 + a, s * 12 + a * 4 + 3] = 1.0
    return m.reshape(384, 256)


def zrows_kernel(e_ref, g_ref, p_ref, o_ref, lo_ref, hi_ref, t_ref):
    e = e_ref[0]
    lane = lax.broadcasted_iota(jnp.int32, (4, 128), 1)
    for d in range(3):
        at = lax.rem(e + (0, 3, 1)[d], 4)
        for j in range(16):
            r, off = divmod(72 * j, 128)
            v = g_ref[at, pl.ds(r, 4, stride=9), :]
            v = pltpu.roll(v, (128 - off) % 128, axis=1) if off else v
            if off + 72 > 128:
                n = g_ref[at, pl.ds(r + 1, 4, stride=9), :]
                n = pltpu.roll(n, 128 - off, axis=1)
                v = jnp.where(lane < 128 - off, v, n)
            r, off = divmod(24 * j, 128)
            k = g_ref[at, pl.ds(36 + r, 4, stride=3), :]
            k = pltpu.roll(k, (72 - off) % 128, axis=1)
            if off + 24 > 128:
                n = g_ref[at, pl.ds(37 + r, 4, stride=3), :]
                n = pltpu.roll(n, (72 - off) % 128, axis=1)
                k = jnp.where(lane < 72 + 128 - off, k, n)
            v = jnp.where(lane < 72, v, jnp.where(lane < 96, k, 0.0))
            t_ref[d, pl.ds(j, 4, stride=16), :] = v
    rows = jnp.concatenate([t_ref[0], t_ref[1], t_ref[2]], axis=1)
    r = mm(jnp.concatenate(split(rows, 3), axis=0), p_ref[...])
    r = (r[0:64] + r[64:128]) + r[128:192]
    for h in range(2):
        v = r[:, 128 * h : 128 * h + 128]
        o_ref[h] = v
        lo_ref[h] = v[0:16]
        hi_ref[h] = v[48:64]


def yslab_kernel(o_ref, m_ref, p_ref, lo_ref, hi_ref):
    for out, base in ((lo_ref, 0), (hi_ref, 6)):
        for h in range(2):
            for k in range(2):
                out[h, 8 * k : 8 * k + 8, :] = o_ref[h, pl.ds(base + k, 8, stride=8), :]
                out[h, 16 + 4 * k : 18 + 4 * k, :] = m_ref[h, pl.ds(base + k, 2, stride=8), :]
                out[h, 18 + 4 * k : 20 + 4 * k, :] = p_ref[h, pl.ds(base + k, 2, stride=8), :]


def weights_kernel(w2, wl, we, wo, ro, t2, tl, te, to, bo, be, bl, b2, rc):
    def three(w):
        h, l = split(w, 2)
        return jnp.concatenate([h, h, l], axis=1)

    pad = jnp.concatenate([w2[...], jnp.zeros((4, 64), F32)], axis=0)
    t2[...] = three(pad.T)
    tl[...] = three(wl[...].T)
    te[...] = three(we[...].T)
    to[...] = three(wo[...].T)
    bo[...] = three(wo[...])
    be[...] = three(we[...])
    bl[...] = three(wl[...])
    b2[...] = three(w2[4:12, :])
    eye = lax.broadcasted_iota(jnp.int32, (64, 64), 0) == lax.broadcasted_iota(
        jnp.int32, (64, 64), 1
    )
    rc[...] = jnp.sum(jnp.where(eye, jnp.broadcast_to(ro[...], (64, 64)), 0.0), axis=1, keepdims=True)


def index_kernel(alive_ref, nb_ref, ce_ref, ct_ref, oh_ref, geo_ref):
    nb = nb_ref[...].astype(F32)
    ce = ce_ref[...].astype(F32)

    def div(v, k):
        return jnp.floor((v + 0.5) * (1.0 / k))

    pq = div(nb, 36)
    r = nb - 36.0 * pq
    p = div(pq, 12)
    q = pq - 12.0 * p
    s = div(r, 3)
    a = r - 3.0 * s
    inx = (p >= 2.0) & (p < 10.0)
    px = jnp.where(p < 2.0, p, p - 8.0)
    row_in = jnp.where(inx, (p - 2.0) * 8.0, jnp.where(p < 2.0, 64.0 + 8.0 * p, 80.0 + 8.0 * (p - 10.0)))
    row_in = row_in + (q - 2.0)
    qy = jnp.where(q < 2.0, q, q - 10.0)
    row_y = jnp.where(inx, 8.0 * qy + (p - 2.0), 16.0 + 4.0 * qy + px)
    row = jnp.where(q < 2.0, 96.0 + row_y, jnp.where(q < 10.0, row_in, 120.0 + row_y))

    cell = div(ce, 3)
    ca = ce - 3.0 * cell
    cxy = div(cell, 8)
    cz = cell - 8.0 * cxy
    cx = div(cxy, 8)
    cy = cxy - 8.0 * cx
    cr = (cz + 2.0) * 3.0 + ca

    def place(x, y, z, atom):
        return (
            x + jnp.where(atom == 1.0, 0.75, 0.25),
            y + jnp.where(atom >= 1.0, 0.75, 0.25),
            z + jnp.where(atom == 2.0, 0.75, 0.25),
        )

    second = place(p - 2.0, q - 2.0, s - 2.0, a)
    first = place(cx, cy, cz, ca)
    for k in range(3):
        geo_ref[k : k + 1, 0:PAIRS] = second[k] - jnp.concatenate([first[k]] * 4, axis=1)
    lane = lax.broadcasted_iota(jnp.int32, (1, PAIRS), 1)
    slot = lax.shift_right_logical(lane, 4)
    centre = lane & 15
    count = jnp.concatenate([ct_ref[...]] * 4, axis=1)
    live = (slot < count) & (centre < alive_ref[0])
    geo_ref[3:4, 0:PAIRS] = jnp.where(live, 1.0, 0.0)
    rows = jnp.concatenate([row, cxy], axis=1)
    geo_ref[4:5, :] = jnp.concatenate([r, cr], axis=1)
    at = lax.broadcasted_iota(jnp.int32, (LANES, PAIRS + 128), 0).astype(F32)
    oh_ref[...] = jnp.where(at == rows, 1.0, 0.0).astype(BF16)


def poly(x, coefs):
    acc = jnp.full_like(x, coefs[-1])
    for c in coefs[-2::-1]:
        acc = acc * x + c
    return acc


SIN = [math.pi ** (2 * k + 1) * (-1) ** k / math.factorial(2 * k + 1) for k in range(7)]
COS = [math.pi ** (2 * k) * (-1) ** k / math.factorial(2 * k) for k in range(8)]
R3, R5, R15 = math.sqrt(3.0), math.sqrt(5.0), math.sqrt(15.0)
ORDER = (0, 1, 1, 1, 2, 2, 2, 2, 2)


def stack3(v):
    h, l = split(v, 2)
    return jnp.concatenate([h, l, h], axis=0)


def slots_sum(v):
    t = (v[:, 0:128] + v[:, 128:256]) + (v[:, 256:384] + v[:, 384:512])
    for by in (16, 32, 64):
        t = t + pltpu.roll(t, by, axis=1)
    return t


def four(v):
    return jnp.concatenate([v] * 4, axis=1)


def main_kernel(
    oh_ref, geo_ref, o_ref, xm_ref, xp_ref, ym_ref, yp_ref,
    t2, tl, te, to, bo, be, bl, b2, rc,
    en_ref, fo_ref, fxm_ref, fxp_ref, fym_ref, fyp_ref,
    w_s, q_s, g_s, a_s, in_s, dw_s, sc_s,
):
    refs = (o_ref, xm_ref, xp_ref, ym_ref, yp_ref)
    tt = jnp.concatenate(
        [
            jnp.concatenate([v[0] for v in refs], axis=0).T,
            jnp.concatenate([v[1] for v in refs], axis=0).T[0 : LANES - 128],
        ],
        axis=0,
    )
    hot = oh_ref[...]
    got = mm(jnp.concatenate(split(tt, 2), axis=0), hot)
    rsel = geo_ref[4:5, :]
    sub = lax.broadcasted_iota(jnp.int32, (8, PAIRS + 128), 0)
    half = lax.shift_right_logical(sub, 2).astype(F32)
    pick = jnp.zeros((8, PAIRS + 128), F32)
    for k in range(18):
        v = got[8 * k : 8 * k + 8] + got[LANES + 8 * k : LANES + 8 * k + 8]
        pick = jnp.where(half + 2.0 * k == rsel, v, pick)
    pick = pick[0:4] + pick[4:8]
    first = four(pick[:, PAIRS:])
    second = pick[:, 0:PAIRS]
    geo = geo_ref[...]
    live = geo[3:4, 0:PAIRS]
    rx = [(geo[k : k + 1, 0:PAIRS] + (second[k : k + 1] - first[k : k + 1])) * CELL for k in range(3)]
    d2 = rx[0] * rx[0] + rx[1] * rx[1] + rx[2] * rx[2]
    inv = lax.rsqrt(d2)
    inv = inv * (1.5 - 0.5 * d2 * inv * inv)
    dist = d2 * inv
    ux, uy, uz = [v * inv for v in rx]
    x = dist * (1.0 / CUT)
    inside = x < 1.0
    x = jnp.minimum(x, 1.0)
    x2 = x * x
    x3 = x2 * x
    x5 = x3 * x2
    x6 = x3 * x3
    env = jnp.where(inside, 1.0 + x6 * (-28.0 + x * (48.0 - 21.0 * x)), 0.0)
    denv_dd = jnp.where(inside, (-168.0 / CUT) * x5 * (1.0 - x) * (1.0 - x), 0.0)
    ev = env * live

    n = (lax.broadcasted_iota(jnp.int32, (8, PAIRS), 0) + 1).astype(F32)
    t = n * x
    k = jnp.floor(t + 0.5)
    f = t - k
    sign = 1.0 - 2.0 * (k - 2.0 * jnp.floor(k * 0.5))
    f2 = f * f
    sn = sign * f * poly(f2, SIN)
    cs = sign * poly(f2, COS)
    c0 = math.sqrt(2.0 / CUT)
    sd = sn * (c0 * inv)
    basis = sd * env
    dbasis = (n * cs) * ((c0 * math.pi / CUT) * inv * env) + sd * (denv_dd - env * inv)
    k1, k2 = first[3:4], second[3:4]
    in_s[0:1, :] = jnp.where(k1 == 0.0, 1.0, 0.0)
    in_s[1:2, :] = jnp.where(k1 == 1.0, 1.0, 0.0)
    in_s[2:3, :] = jnp.where(k2 == 0.0, 1.0, 0.0)
    in_s[3:4, :] = jnp.where(k2 == 1.0, 1.0, 0.0)
    in_s[4:12, :] = basis
    in_s[12:16, :] = jnp.zeros((4, PAIRS), F32)

    def silu(v):
        sg = 1.0 / (1.0 + jnp.exp(-v))
        return v * sg, sg * (1.0 + v * (1.0 - sg))

    h, dh_ = silu(mm(t2[...], stack3(in_s[...])))
    z, dz_ = silu(mm(tl[...], stack3(h)))
    zs = stack3(z)
    e = mm(te[...], zs)
    w_s[...] = e * ev

    ys = [
        None, R3 * ux, R3 * uy, R3 * uz, R15 * ux * uy, R15 * uy * uz,
        (0.5 * R5) * (3.0 * uz * uz - 1.0), R15 * ux * uz, (0.5 * R15) * (ux * ux - uy * uy),
    ]
    yb = [None] + [jnp.broadcast_to(v, (8, PAIRS)) for v in ys[1:]]
    for c in range(8):
        at = slice(8 * c, 8 * c + 8)
        w = w_s[at, :]
        sums = [None, None, None]
        for m in range(9):
            am = 0.2 * slots_sum(w if m == 0 else w * yb[m])
            a_s[m, at, :] = am
            am = four(am)
            term = am if m == 0 else yb[m] * am
            l = ORDER[m]
            sums[l] = term if sums[l] is None else sums[l] + term
        for l in range(3):
            q_s[l, at, :] = sums[l]
    wv = w_s[...]
    joined = jnp.concatenate([z] + [wv * q_s[l] for l in range(3)], axis=0)
    y, dy_ = silu(mm(to[...], stack3(joined)))
    ro = rc[...]
    raw = jnp.sum(ro * y, axis=0, keepdims=True)
    en = slots_sum(raw * ev)
    en_ref[...] = en[:, 0:NS].reshape(1, 1, NS)
    denv = live * raw
    dj = mm(bo[...], stack3((ro * ev) * dy_))
    g_s[...] = dj[64:256]
    acc = [None] * 9
    for c in range(8):
        at = slice(8 * c, 8 * c + 8)
        w = w_s[at, :]
        dw = None
        for l in range(3):
            g = g_s[64 * l + 8 * c : 64 * l + 8 * c + 8, :]
            part = g * q_s[l, at, :]
            dw = part if dw is None else dw + part
            gw = g * w
            for m in range(9):
                if ORDER[m] != l:
                    continue
                bm = four(0.2 * slots_sum(gw if m == 0 else gw * yb[m]))
                dw = dw + (bm if m == 0 else yb[m] * bm)
                if m:
                    v = gw * four(a_s[m, at, :]) + w * bm
                    acc[m] = v if acc[m] is None else acc[m] + v
        dw_s[at, :] = dw
    dw = dw_s[...]
    denv = denv + live * jnp.sum(dw * e, axis=0, keepdims=True)
    dz = dj[0:64] + mm(be[...], stack3(dw * ev))
    dh = mm(bl[...], stack3(dz * dz_))
    db = mm(b2[...], stack3(dh * dh_))
    dd = denv * denv_dd + jnp.sum(db * dbasis, axis=0, keepdims=True)
    dy = [None] + [jnp.sum(acc[m], axis=0, keepdims=True) for m in range(1, 9)]
    du0 = R3 * dy[1] + R15 * (uy * dy[4] + uz * dy[7] + ux * dy[8])
    du1 = R3 * dy[2] + R15 * (ux * dy[4] + uz * dy[5] - uy * dy[8])
    du2 = R3 * dy[3] + R15 * (uy * dy[5] + ux * dy[7]) + (3.0 * R5) * uz * dy[6]
    along = ux * du0 + uy * du1 + uz * du2
    dd = dd - along * inv
    grad = [du0 * inv + ux * dd, du1 * inv + uy * dd, du2 * inv + uz * dd]

    lane = lax.broadcasted_iota(jnp.int32, (1, 128), 1)
    sc_s[...] = jnp.zeros((8, PAIRS + 128), F32)
    for k in range(3):
        own = jnp.where(lane < NS, slots_sum(grad[k]), 0.0)
        for row in (k, k + 4):
            sc_s[row : row + 1, 0:PAIRS] = -grad[k]
            sc_s[row : row + 1, PAIRS:] = own
    gv = sc_s[...]
    m = jnp.concatenate(
        [jnp.where(half + 2.0 * k == rsel, gv, 0.0) for k in range(18)]
        + [jnp.zeros((256 - LANES, PAIRS + 128), F32)],
        axis=0,
    )
    mh, ml = split(m, 2)
    nt = ((1,), (1,))
    out = mm(hot, mh, nt) + mm(hot, ml, nt)
    for h in range(2):
        v = out[:, 128 * h : 128 * h + 128]
        fo_ref[h] = v[0:64]
        fxm_ref[h] = v[64:80]
        fxp_ref[h] = v[80:96]
        fym_ref[h] = v[96:120]
        fyp_ref[h] = v[120:144]


def yfold_kernel(fo, fm, fp, lo, hi, o_ref, m_ref, p_ref):
    o_ref[...] = fo[...]
    m_ref[...] = fm[...]
    p_ref[...] = fp[...]
    for got, base in ((lo, 0), (hi, 6)):
        for k in range(2):
            for ref, a, n in ((o_ref, 8 * k, 8), (m_ref, 16 + 4 * k, 2), (p_ref, 18 + 4 * k, 2)):
                at = pl.ds(base + k, n, stride=8)
                for h in range(2):
                    ref[h, at, :] = ref[h, at, :] + got[h, a : a + n, :]


def xfold_kernel(fo, lo, hi, o_ref, z_ref):
    a, b = [
        jnp.concatenate([fo[h, 0:16, :] + lo[h], fo[h, 16:48, :], fo[h, 48:64, :] + hi[h]], axis=0)
        for h in range(2)
    ]
    o_ref[...] = a
    lane = lax.broadcasted_iota(jnp.int32, (64, 128), 1)
    b = pltpu.roll(b, 24, axis=1)
    z_ref[...] = jnp.where(
        lane < 24, a, jnp.where(lane < 40, b, jnp.where(lane < 120, 0.0, a))
    )


def fperm():
    m = np.zeros((128, 128), np.float32)
    for z in range(8):
        for a in range(3):
            for c in range(3):
                m[24 + z * 12 + a * 4 + c, z * 9 + a * 3 + c] = 1.0
    return m


def zfold_kernel(e_ref, f_ref, g_ref, p_ref, o_ref, t_ref):
    e = e_ref[0]
    lane = lax.broadcasted_iota(jnp.int32, (64, 128), 1)
    above = g_ref[lax.rem(e + 1, 4)]
    below = g_ref[lax.rem(e + 3, 4)]
    f = f_ref[...]
    f = f + jnp.where((lane >= 96) & (lane < 120), pltpu.roll(above, 96, axis=1), 0.0)
    low = jnp.where(lane < 32, pltpu.roll(below, 32, axis=1), pltpu.roll(below, 8, axis=1))
    f = f + jnp.where((lane >= 24) & (lane < 48), low, 0.0)
    r = mm(jnp.concatenate(split(f, 3), axis=0), p_ref[...])
    t_ref[...] = (r[0:64] + r[64:128]) + r[128:192]
    lane = lax.broadcasted_iota(jnp.int32, (4, 128), 1)
    for k in range(9):
        v = jnp.zeros((4, 128), F32)
        for j in range(128 * k // 72, (128 * k + 127) // 72 + 1):
            off = 72 * j - 128 * k
            part = pltpu.roll(t_ref[pl.ds(j, 4, stride=16), :], off % 128, axis=1)
            v = v + jnp.where((lane >= off) & (lane < off + 72), part, 0.0)
        for g in range(4):
            o_ref[0, :, 128 * (9 * g + k) : 128 * (9 * g + k) + 128] = v[g : g + 1]


def sds(shape, dtype=F32):
    return jax.ShapeDtypeStruct(shape, dtype)


def hop(v, axis, by):
    n = lax.axis_size(axis)
    return lax.ppermute(v, axis, [(i, (i + by) % n) for i in range(n)])


def local(
    displacement, species, centres, neighbours, neighbour_count, live_centres,
    w_two, w_lat, w_env, w_out, readout,
):
    e = lax.axis_index("gz").astype(jnp.int32).reshape(1)
    flat = call(pack_kernel, sds((48, 128)), [(displacement, VM), (species, VM)], "pack")
    column = lax.all_gather(flat, "gz")
    slab = sds((2, 16, 128))
    own, lo, hi = call(
        zrows_kernel,
        (sds((2, 64, 128)), slab, slab),
        [(e, SM), (column, VM), (jnp.asarray(zperm(), BF16), VM)],
        "zrows",
        [pltpu.VMEM((3, 64, 128), F32)],
    )
    xm, xp = hop(hi, "gx", 1), hop(lo, "gx", -1)

    ws = call(
        weights_kernel,
        (
            sds((64, 48), BF16), sds((64, 192), BF16), sds((64, 192), BF16), sds((64, 768), BF16),
            sds((256, 192), BF16), sds((64, 192), BF16), sds((64, 192), BF16), sds((8, 192), BF16),
            sds((64, 1)),
        ),
        [(w_two, VM), (w_lat, VM), (w_env, VM), (w_out, VM), (readout.reshape(1, 64), VM)],
        "weights",
    )
    hot, geo = call(
        index_kernel,
        (sds((LANES, PAIRS + 128), BF16), sds((8, PAIRS + 128))),
        [
            (live_centres.reshape(1), SM),
            (neighbours.reshape(NS, 32).T.reshape(1, PAIRS), VM),
            (jnp.tile(centres.reshape(1, NS), (1, 8)), VM),
            (jnp.tile(neighbour_count.reshape(1, NS), (1, 8)), VM),
        ],
        "index",
    )

    slab = sds((2, 24, 128))
    lo, hi = call(yslab_kernel, (slab, slab), [(own, VM), (xm, VM), (xp, VM)], "yslab")
    ym, yp = hop(hi, "gy", 1), hop(lo, "gy", -1)

    en, fo, fxm, fxp, fym, fyp = call(
        main_kernel,
        (
            sds((1, 1, NS)), sds((2, 64, 128)), sds((2, 16, 128)), sds((2, 16, 128)),
            sds((2, 24, 128)), sds((2, 24, 128)),
        ),
        [(v, VM) for v in (hot, geo, own, xm, xp, ym, yp, *ws)],
        "pairs",
        [
            pltpu.VMEM((64, PAIRS), F32), pltpu.VMEM((3, 64, PAIRS), F32),
            pltpu.VMEM((192, PAIRS), F32), pltpu.VMEM((9, 64, 128), F32),
            pltpu.VMEM((16, PAIRS), F32), pltpu.VMEM((64, PAIRS), F32),
            pltpu.VMEM((8, PAIRS + 128), F32),
        ],
    )
    hi, lo = hop(fym, "gy", -1), hop(fyp, "gy", 1)
    fo, fxm, fxp = call(
        yfold_kernel,
        (sds((2, 64, 128)), sds((2, 16, 128)), sds((2, 16, 128))),
        [(v, VM) for v in (fo, fxm, fxp, lo, hi)],
        "yfold",
    )
    hi, lo = hop(fxm, "gx", -1), hop(fxp, "gx", 1)
    fo, z = call(
        xfold_kernel, (sds((64, 128)), sds((64, 128))), [(fo, VM), (lo, VM), (hi, VM)], "xfold"
    )
    column = lax.all_gather(z, "gz")
    out = call(
        zfold_kernel,
        sds((1, 1, 4608)),
        [(e, SM), (fo, VM), (column, VM), (jnp.asarray(fperm(), BF16), VM)],
        "zfold",
        [pltpu.VMEM((64, 128), F32)],
    )
    return en, out


def solution(mesh):
    cut = P("gx", "gy", "gz")
    return jax.shard_map(
        local,
        mesh=mesh,
        in_specs=(cut,) * 6 + (P(),) * 5,
        out_specs=(cut, cut),
        check_vma=False,
    )
```

```python
import math

import jax
import jax.numpy as jnp
import numpy as np
from jax import lax
from jax.experimental import pallas as pl
from jax.experimental.pallas import tpu as pltpu
from jax.sharding import PartitionSpec as P

F32 = jnp.float32
BF16 = jnp.bfloat16
CELL = 3.1
CUT = 6.0
VM = pl.BlockSpec(memory_space=pltpu.VMEM)
SM = pl.BlockSpec(memory_space=pltpu.SMEM)
PAIRS = 512
NS = 16
LIST = 40


def call(kernel, outs, ins, name, scratch=(), flops=0, mib=2):
    specs = [s for _, s in ins]
    return pl.pallas_call(
        kernel,
        out_shape=outs,
        in_specs=specs,
        out_specs=jax.tree.map(lambda _: VM, outs),
        scratch_shapes=list(scratch),
        name=name,
        compiler_params=pltpu.CompilerParams(vmem_limit_bytes=mib << 20),
        cost_estimate=pl.CostEstimate(flops=flops, bytes_accessed=0, transcendentals=0),
    )(*[a for a, _ in ins])


def split(v, parts):
    out = []
    for _ in range(parts - 1):
        h = v.astype(BF16)
        out.append(h)
        v = v - h.astype(F32)
    out.append(v.astype(BF16))
    return out


def mm(a, b, dims=((1,), (0,))):
    return lax.dot_general(a, b, (dims, ((), ())), preferred_element_type=F32)


def pack_kernel(d_ref, s_ref, nb_ref, ce_ref, ct_ref, al_ref, o_ref, t_ref):
    for i in range(36):
        o_ref[i : i + 1, :] = d_ref[0, :, 128 * i : 128 * i + 128]
    for i in range(12):
        o_ref[36 + i : 37 + i, :] = s_ref[0, :, 128 * i : 128 * i + 128].astype(F32)
    o_ref[48 : 48 + LIST, :] = jnp.zeros((LIST, 128), F32)
    t_ref[...] = jnp.zeros((128, 128), F32)
    for i in range(4):
        v = nb_ref[0, :, 128 * i : 128 * i + 128].astype(F32)
        for c in range(4):
            t_ref[4 * i + c : 4 * i + c + 1, :] = pltpu.roll(v, (128 - 32 * c) % 128, axis=1)
    o_ref[48:80, 0:NS] = t_ref[...].T[0:32, 0:NS]
    lane = lax.broadcasted_iota(jnp.int32, (1, NS), 1)
    o_ref[80:81, 0:NS] = ce_ref[0].astype(F32)
    o_ref[81:82, 0:NS] = jnp.where(lane < al_ref[0], ct_ref[0], 0).astype(F32)


def zperm():
    m = np.zeros((3, 128, 256), np.float32)
    for s in range(16):
        d, z = (1, s + 4) if s < 4 else ((0, s - 4) if s < 12 else (2, s - 12))
        for a in range(3):
            at = (s // 8) * 128 + (s % 8) * 12 + a * 4
            for c in range(3):
                m[d, z * 9 + a * 3 + c, at + c] = 1.0
            m[d, 72 + z * 3 + a, at + 3] = 1.0
    return m.reshape(384, 256)


def zrows_kernel(e_ref, g_ref, p_ref, o_ref, l_ref, lo_ref, hi_ref, t_ref):
    e = e_ref[0]
    lane = lax.broadcasted_iota(jnp.int32, (4, 128), 1)
    wide = lax.broadcasted_iota(jnp.int32, (LIST, 128), 1)
    lists = jnp.zeros((LIST, 128), F32)
    for d in range(3):
        at = lax.rem(e + (0, 3, 1)[d], 4)
        for j in range(16):
            r, off = divmod(72 * j, 128)
            v = g_ref[at, pl.ds(r, 4, stride=9), :]
            v = pltpu.roll(v, (128 - off) % 128, axis=1) if off else v
            if off + 72 > 128:
                n = g_ref[at, pl.ds(r + 1, 4, stride=9), :]
                n = pltpu.roll(n, 128 - off, axis=1)
                v = jnp.where(lane < 128 - off, v, n)
            r, off = divmod(24 * j, 128)
            k = g_ref[at, pl.ds(36 + r, 4, stride=3), :]
            k = pltpu.roll(k, (72 - off) % 128, axis=1)
            if off + 24 > 128:
                n = g_ref[at, pl.ds(37 + r, 4, stride=3), :]
                n = pltpu.roll(n, (72 - off) % 128, axis=1)
                k = jnp.where(lane < 72 + 128 - off, k, n)
            v = jnp.where(lane < 72, v, jnp.where(lane < 96, k, 0.0))
            t_ref[d, pl.ds(j, 4, stride=16), :] = v
        b = NS * (1, 0, 2)[d]
        v = g_ref[at, 48 : 48 + LIST, :]
        v = pltpu.roll(v, b, axis=1) if b else v
        lists = jnp.where((wide >= b) & (wide < b + NS), v, lists)
    rows = jnp.concatenate([t_ref[0], t_ref[1], t_ref[2]], axis=1)
    r = mm(jnp.concatenate(split(rows, 3), axis=0), p_ref[...])
    r = (r[0:64] + r[64:128]) + r[128:192]
    l_ref[...] = lists
    for h in range(2):
        v = r[:, 128 * h : 128 * h + 128]
        o_ref[h] = v
        lo_ref[32 * h : 32 * h + 32, :] = v[0:32]
        hi_ref[32 * h : 32 * h + 32, :] = v[32:64]
    lo_ref[64 : 64 + LIST, :] = lists
    hi_ref[64 : 64 + LIST, :] = lists


def yslab_kernel(o_ref, l_ref, m_ref, p_ref, la_ref, lo_ref, hi_ref):
    lane = lax.broadcasted_iota(jnp.int32, (LIST, 128), 1)
    first = jnp.where(lane < 48, l_ref[...], pltpu.roll(m_ref[64 : 64 + LIST, :], 48, axis=1))
    second = p_ref[64 : 64 + LIST, :]
    la_ref[0:LIST, :] = first
    la_ref[LIST : 2 * LIST, :] = second
    for out, base in ((lo_ref, 0), (hi_ref, 4)):
        for h in range(2):
            for k in range(4):
                at = 64 * h + 16 * k
                out[at : at + 8, :] = o_ref[h, pl.ds(base + k, 8, stride=8), :]
                out[at + 8 : at + 12, :] = m_ref[pl.ds(32 * h + base + k, 4, stride=8), :]
                out[at + 12 : at + 16, :] = p_ref[pl.ds(32 * h + base + k, 4, stride=8), :]
        out[128 : 128 + LIST, :] = first
        out[128 + LIST : 128 + 2 * LIST, :] = second


def weights_kernel(w2, wl, we, wot, ro, t2, tl, te, to, bo, be, bl, b2, rc):
    def three(w):
        h, l = split(w, 2)
        return jnp.concatenate([h, h, l], axis=1)

    pad = jnp.concatenate([w2[...], jnp.zeros((4, 64), F32)], axis=0)
    t2[...] = three(pad.T)
    tl[...] = three(wl[...].T)
    te[...] = three(we[...].T)
    to[...] = three(wot[...])
    bo[...] = three(wot[...].T)
    be[...] = three(we[...])
    bl[...] = three(wl[...])
    b2[...] = three(w2[4:12, :])
    eye = lax.broadcasted_iota(jnp.int32, (64, 64), 0) == lax.broadcasted_iota(
        jnp.int32, (64, 64), 1
    )
    rc[...] = jnp.sum(jnp.where(eye, jnp.broadcast_to(ro[...], (64, 64)), 0.0), axis=1, keepdims=True)


def poly(x, coefs):
    acc = jnp.full_like(x, coefs[-1])
    for c in coefs[-2::-1]:
        acc = acc * x + c
    return acc


SIN = [math.pi ** (2 * k + 1) * (-1) ** k / math.factorial(2 * k + 1) for k in range(7)]
COS = [math.pi ** (2 * k) * (-1) ** k / math.factorial(2 * k) for k in range(8)]
R3, R5, R15 = math.sqrt(3.0), math.sqrt(5.0), math.sqrt(15.0)
ORDER = (0, 1, 1, 1, 2, 2, 2, 2, 2)


def stack3(v):
    h, l = split(v, 2)
    return jnp.concatenate([h, l, h], axis=0)


def slots_sum(v):
    t = (v[:, 0:128] + v[:, 128:256]) + (v[:, 256:384] + v[:, 384:512])
    for by in (16, 32, 64):
        t = t + pltpu.roll(t, by, axis=1)
    return t


def four(v):
    return jnp.concatenate([v] * 4, axis=1)


def div(v, k):
    return jnp.floor((v + 0.5) * (1.0 / k))


def cell_of(ce):
    cell = div(ce, 3)
    xy = div(cell, 8)
    x = div(xy, 8)
    return x, xy - 8.0 * x, cell - 8.0 * xy, ce - 3.0 * cell


def table_row(p, q):
    px = jnp.where(p < 4.0, p + 8.0, jnp.where(p < 12.0, p - 4.0, p))
    mid = q - 4.0 + 8.0 * jnp.where(p < 4.0, p + 8.0, jnp.where(p < 12.0, p - 4.0, p))
    return jnp.where(q < 4.0, 128.0 + 16.0 * q + px, jnp.where(q < 12.0, mid, 16.0 * q + px))


def place(x, y, z, atom):
    return (
        x + jnp.where(atom == 1.0, 0.75, 0.25),
        y + jnp.where(atom >= 1.0, 0.75, 0.25),
        z + jnp.where(atom == 2.0, 0.75, 0.25),
    )


def fperm():
    m = np.zeros((128, 128), np.float32)
    for z in range(8):
        for a in range(3):
            for c in range(3):
                m[z * 12 + a * 4 + c, z * 9 + a * 3 + c] = 1.0
    return m


def tiles(of):
    lane = lax.broadcasted_iota(jnp.int32, of, 1)
    row = lax.broadcasted_iota(jnp.int32, of, 0) if of[1] == 128 else lax.shift_right_logical(lane, 7)
    lane = lane & 127
    step = lax.shift_right_logical(row, 1)
    second = row & 1
    dy = jnp.where(step == 0, 0, jnp.where(step == 1, -1, 1))
    dx = jnp.where(second == 1, 1, jnp.where(lane < 48, 0, -1))
    at = jnp.where(lane < 48, lane, lane - 48)
    dz = lax.shift_right_logical(at, 4) - 1
    valid = (row < 6) & (lane < jnp.where(second == 1, 48, 96))
    return [v.astype(F32) for v in (dx, dy, dz)], valid, (row == 0) & (lane >= 16) & (lane < 32), lane


def main_kernel(
    o_ref, la_ref, xm_ref, xp_ref, ym_ref, yp_ref,
    t2, tl, te, to, bo, be, bl, b2, rc, fp_ref,
    en_ref, fo_ref,
    w_s, q_s, g_s, a_s, in_s, dw_s, sc_s, tb_s, ls_s, rk_s, acc_s, out_s,
):
    halves = []
    for h in range(2):
        v = jnp.concatenate(
            [
                o_ref[h], xm_ref[32 * h : 32 * h + 32, :], xp_ref[32 * h : 32 * h + 32, :],
                ym_ref[64 * h : 64 * h + 64, :], yp_ref[64 * h : 64 * h + 64, :],
            ],
            axis=0,
        )
        halves.append(v.T[0:96])
    tb_s[...] = jnp.concatenate(split(jnp.concatenate(halves, axis=0), 2), axis=0)

    places = [(la_ref, 0), (la_ref, LIST), (ym_ref, 128), (ym_ref, 128 + LIST), (yp_ref, 128), (yp_ref, 128 + LIST)]
    (dx, dy, dz), _, _, _ = tiles((1, 768))
    lst = jnp.concatenate([ref[at : at + LIST, :] for ref, at in places], axis=1)
    high = jnp.floor(lst[0:33] * (1.0 / 64.0))
    low = lst[0:33] - 64.0 * high
    ls_s[...] = jnp.concatenate(
        [
            high[0:32], low[0:32], high[32:33], low[32:33], lst[33:34],
            dx + 1.0, dy + 1.0, dz + 1.0, jnp.zeros((10, 768), F32),
        ],
        axis=0,
    ).astype(BF16)
    (dx, dy, dz), valid, own, lane = tiles((8, 128))
    pad = jnp.zeros((2, 128), F32)
    ce = jnp.concatenate([ref[at + 32 : at + 33, :] for ref, at in places] + [pad], axis=0)
    ct = jnp.concatenate([ref[at + 33 : at + 34, :] for ref, at in places] + [pad], axis=0)
    cx, cy, cz, _ = cell_of(ce)
    flag = valid & (~own) & (ct > 0.0)
    for c, d in ((cx, dx), (cy, dy), (cz, dz)):
        v = c + 8.0 * d
        flag = flag & (v >= -2.0) & (v < 10.0)
    flag = jnp.where(flag, 1.0, 0.0)
    tri = lax.broadcasted_iota(jnp.int32, (128, 128), 0) <= lax.broadcasted_iota(
        jnp.int32, (128, 128), 1
    )
    upto = mm(flag.astype(BF16), jnp.where(tri, 1.0, 0.0).astype(BF16))
    total = jnp.broadcast_to(jnp.sum(flag, axis=1, keepdims=True), (8, 128))
    row = lax.broadcasted_iota(jnp.int32, (8, 128), 0)
    before = jnp.where(row >= 1, pltpu.roll(total, 1, axis=0), 0.0)
    for by in (1, 2, 4):
        before = before + jnp.where(row >= by, pltpu.roll(before, by, axis=0), 0.0)
    rank = jnp.where(flag > 0.0, upto + before + (NS - 1.0), -1.0)
    rk_s[...] = jnp.where(own, (lane - 16).astype(F32), rank)
    ghosts = jnp.sum(flag).astype(jnp.int32)
    blocks = 1 + lax.shift_right_logical(ghosts + (NS - 1), 4)
    acc_s[...] = jnp.zeros((64, 128), F32)
    sc_s[...] = jnp.zeros((8, PAIRS + 128), F32)
    in_s[12:16, :] = jnp.zeros((4, PAIRS), F32)

    def block(b, carry):
        want = (lax.broadcasted_iota(jnp.int32, (128, 128), 0) & 15) + NS * b
        want = want.astype(F32)
        chosen = jnp.concatenate(
            [jnp.where(want == rk_s[t : t + 1, :], 1.0, 0.0).astype(BF16) for t in range(6)], axis=1
        )
        u = mm(ls_s[...], chosen, ((1,), (1,)))
        sub = lax.broadcasted_iota(jnp.int32, (8, 128), 0)
        mine = sub == lax.shift_right_logical(lax.broadcasted_iota(jnp.int32, (8, 128), 1), 4)

        def slots(at):
            return jnp.concatenate(
                [
                    jnp.sum(jnp.where(mine, u[at + 8 * g : at + 8 * g + 8], 0.0), axis=0, keepdims=True)
                    for g in range(4)
                ],
                axis=1,
            )

        nb = 64.0 * slots(0) + slots(32)
        ce = 64.0 * u[64:65] + u[65:66]
        count = u[66:67]
        shift = [8.0 * (u[67 + k : 68 + k] - 1.0) for k in range(3)]
        cx, cy, cz, ca = cell_of(ce)
        cx, cy, cz = cx + shift[0], cy + shift[1], cz + shift[2]
        pq = div(nb, 36)
        r = nb - 36.0 * pq
        p = div(pq, 12)
        q = pq - 12.0 * p
        s = div(r, 3)
        a = r - 3.0 * s
        p = p + four(shift[0] - 2.0)
        q = q + four(shift[1] - 2.0)
        s = s + four(shift[2] - 2.0)
        lane = lax.broadcasted_iota(jnp.int32, (1, PAIRS), 1)
        alive = lax.shift_right_logical(lane, 4).astype(F32) < four(count)
        live = jnp.where(alive, 1.0, 0.0)
        second = place(p, q, s, a)
        centre = place(cx, cy, cz, ca)
        geo = [second[k] - four(centre[k]) for k in range(3)]
        rows = jnp.concatenate([table_row(p + 4.0, q + 4.0), table_row(cx + 4.0, cy + 4.0)], axis=1)
        rsel = jnp.concatenate([3.0 * (s + 4.0) + a, 3.0 * (cz + 4.0) + ca], axis=1)
        at = lax.broadcasted_iota(jnp.int32, (256, PAIRS + 128), 0).astype(F32)
        hot = jnp.where(at == rows, 1.0, 0.0).astype(BF16)

        got = mm(tb_s[...], hot)
        half = lax.shift_right_logical(
            lax.broadcasted_iota(jnp.int32, (8, PAIRS + 128), 0), 2
        ).astype(F32)
        pick = jnp.zeros((8, PAIRS + 128), F32)
        for k in range(24):
            v = got[8 * k : 8 * k + 8] + got[192 + 8 * k : 200 + 8 * k]
            pick = jnp.where(half + 2.0 * k == rsel, v, pick)
        pick = pick[0:4] + pick[4:8]
        first = four(pick[:, PAIRS:])
        second = pick[:, 0:PAIRS]
        rx = [
            jnp.where(alive, (geo[k] + (second[k : k + 1] - first[k : k + 1])) * CELL, 1.0)
            for k in range(3)
        ]
        d2 = rx[0] * rx[0] + rx[1] * rx[1] + rx[2] * rx[2]
        inv = lax.rsqrt(d2)
        inv = inv * (1.5 - 0.5 * d2 * inv * inv)
        dist = d2 * inv
        ux, uy, uz = [v * inv for v in rx]
        x = dist * (1.0 / CUT)
        inside = x < 1.0
        x = jnp.minimum(x, 1.0)
        x2 = x * x
        x3 = x2 * x
        x5 = x3 * x2
        x6 = x3 * x3
        env = jnp.where(inside, 1.0 + x6 * (-28.0 + x * (48.0 - 21.0 * x)), 0.0)
        denv_dd = jnp.where(inside, (-168.0 / CUT) * x5 * (1.0 - x) * (1.0 - x), 0.0)
        ev = env * live

        n = (lax.broadcasted_iota(jnp.int32, (8, PAIRS), 0) + 1).astype(F32)
        t = n * x
        k = jnp.floor(t + 0.5)
        f = t - k
        sign = 1.0 - 2.0 * (k - 2.0 * jnp.floor(k * 0.5))
        f2 = f * f
        sn = sign * f * poly(f2, SIN)
        cs = sign * poly(f2, COS)
        c0 = math.sqrt(2.0 / CUT)
        sd = sn * (c0 * inv)
        basis = sd * env
        dbasis = (n * cs) * ((c0 * math.pi / CUT) * inv * env) + sd * (denv_dd - env * inv)
        k1, k2 = first[3:4], second[3:4]
        in_s[0:1, :] = jnp.where(k1 == 0.0, 1.0, 0.0)
        in_s[1:2, :] = jnp.where(k1 == 1.0, 1.0, 0.0)
        in_s[2:3, :] = jnp.where(k2 == 0.0, 1.0, 0.0)
        in_s[3:4, :] = jnp.where(k2 == 1.0, 1.0, 0.0)
        in_s[4:12, :] = basis

        def silu(v):
            sg = 1.0 / (1.0 + jnp.exp(-v))
            return v * sg, sg * (1.0 + v * (1.0 - sg))

        h, dh_ = silu(mm(t2[...], stack3(in_s[...])))
        z, dz_ = silu(mm(tl[...], stack3(h)))
        zs = stack3(z)
        e = mm(te[...], zs)
        w_s[...] = e * ev

        ys = [
            None, R3 * ux, R3 * uy, R3 * uz, R15 * ux * uy, R15 * uy * uz,
            (0.5 * R5) * (3.0 * uz * uz - 1.0), R15 * ux * uz, (0.5 * R15) * (ux * ux - uy * uy),
        ]
        yb = [None] + [jnp.broadcast_to(v, (8, PAIRS)) for v in ys[1:]]
        for c in range(8):
            at = slice(8 * c, 8 * c + 8)
            w = w_s[at, :]
            sums = [None, None, None]
            for m in range(9):
                am = 0.2 * slots_sum(w if m == 0 else w * yb[m])
                a_s[m, at, :] = am
                am = four(am)
                term = am if m == 0 else yb[m] * am
                l = ORDER[m]
                sums[l] = term if sums[l] is None else sums[l] + term
            for l in range(3):
                q_s[l, at, :] = sums[l]
        wv = w_s[...]
        joined = jnp.concatenate([z] + [wv * q_s[l] for l in range(3)], axis=0)
        y, dy_ = silu(mm(to[...], stack3(joined)))
        ro = rc[...]
        raw = jnp.sum(ro * y, axis=0, keepdims=True)
        en = slots_sum(raw * ev)

        @pl.when(b == 0)
        def _():
            en_ref[...] = en[:, 0:NS].reshape(1, 1, NS)

        denv = live * raw
        dj = mm(bo[...], stack3((ro * ev) * dy_))
        g_s[...] = dj[64:256]
        acc = [None] * 9
        for c in range(8):
            at = slice(8 * c, 8 * c + 8)
            w = w_s[at, :]
            dw = None
            for l in range(3):
                g = g_s[64 * l + 8 * c : 64 * l + 8 * c + 8, :]
                part = g * q_s[l, at, :]
                dw = part if dw is None else dw + part
                gw = g * w
                for m in range(9):
                    if ORDER[m] != l:
                        continue
                    bm = four(0.2 * slots_sum(gw if m == 0 else gw * yb[m]))
                    dw = dw + (bm if m == 0 else yb[m] * bm)
                    if m:
                        v = gw * four(a_s[m, at, :]) + w * bm
                        acc[m] = v if acc[m] is None else acc[m] + v
            dw_s[at, :] = dw
        dw = dw_s[...]
        denv = denv + live * jnp.sum(dw * e, axis=0, keepdims=True)
        dz = dj[0:64] + mm(be[...], stack3(dw * ev))
        dh = mm(bl[...], stack3(dz * dz_))
        db = mm(b2[...], stack3(dh * dh_))
        dd = denv * denv_dd + jnp.sum(db * dbasis, axis=0, keepdims=True)
        dy = [None] + [jnp.sum(acc[m], axis=0, keepdims=True) for m in range(1, 9)]
        du0 = R3 * dy[1] + R15 * (uy * dy[4] + uz * dy[7] + ux * dy[8])
        du1 = R3 * dy[2] + R15 * (ux * dy[4] + uz * dy[5] - uy * dy[8])
        du2 = R3 * dy[3] + R15 * (uy * dy[5] + ux * dy[7]) + (3.0 * R5) * uz * dy[6]
        along = ux * du0 + uy * du1 + uz * du2
        dd = dd - along * inv
        grad = [du0 * inv + ux * dd, du1 * inv + uy * dd, du2 * inv + uz * dd]
        for k in range(3):
            mine = jnp.where(lane[:, 0:128] < NS, slots_sum(grad[k]), 0.0)
            for row in (k, k + 4):
                sc_s[row : row + 1, 0:PAIRS] = -grad[k]
                sc_s[row : row + 1, PAIRS:] = mine
        gv = sc_s[...]
        m = jnp.concatenate(
            [jnp.where(half + (12.0 + 2.0 * k) == rsel, gv, 0.0) for k in range(12)]
            + [jnp.zeros((32, PAIRS + 128), F32)],
            axis=0,
        )
        mh, ml = split(m, 2)
        nt = ((1,), (1,))
        acc_s[...] += mm(hot[0:64], mh, nt) + mm(hot[0:64], ml, nt)
        return carry

    lax.fori_loop(0, blocks, block, 0)

    r = mm(jnp.concatenate(split(acc_s[...], 3), axis=0), fp_ref[...])
    out_s[...] = (r[0:64] + r[64:128]) + r[128:192]
    lane = lax.broadcasted_iota(jnp.int32, (4, 128), 1)
    for k in range(9):
        v = jnp.zeros((4, 128), F32)
        for j in range(128 * k // 72, (128 * k + 127) // 72 + 1):
            off = 72 * j - 128 * k
            part = pltpu.roll(out_s[pl.ds(j, 4, stride=16), :], off % 128, axis=1)
            v = v + jnp.where((lane >= off) & (lane < off + 72), part, 0.0)
        for g in range(4):
            fo_ref[0, :, 128 * (9 * g + k) : 128 * (9 * g + k) + 128] = v[g : g + 1]


def sds(shape, dtype=F32):
    return jax.ShapeDtypeStruct(shape, dtype)


def hop(v, axis, by):
    n = lax.axis_size(axis)
    return lax.ppermute(v, axis, [(i, (i + by) % n) for i in range(n)])


def local(
    displacement, species, centres, neighbours, neighbour_count, live_centres,
    w_two, w_lat, w_env, w_out, readout,
):
    e = lax.axis_index("gz").astype(jnp.int32).reshape(1)
    flat = call(
        pack_kernel,
        sds((48 + LIST, 128)),
        [(v, VM) for v in (displacement, species, neighbours, centres, neighbour_count, live_centres)],
        "pack",
        [pltpu.VMEM((128, 128), F32)],
    )
    column = lax.all_gather(flat, "gz")
    slab = sds((64 + LIST, 128))
    own, lists, lo, hi = call(
        zrows_kernel,
        (sds((2, 64, 128)), sds((LIST, 128)), slab, slab),
        [(e, SM), (column, VM), (jnp.asarray(zperm(), BF16), VM)],
        "zrows",
        [pltpu.VMEM((3, 64, 128), F32)],
    )
    xm, xp = hop(hi, "gx", 1), hop(lo, "gx", -1)
    ws = call(
        weights_kernel,
        (
            sds((64, 48), BF16), sds((64, 192), BF16), sds((64, 192), BF16), sds((64, 768), BF16),
            sds((256, 192), BF16), sds((64, 192), BF16), sds((64, 192), BF16), sds((8, 192), BF16),
            sds((64, 1)),
        ),
        [(v, VM) for v in (w_two, w_lat, w_env, w_out.T, readout.reshape(1, 64))],
        "weights",
    )
    slab = sds((128 + 2 * LIST, 128))
    lists, lo, hi = call(
        yslab_kernel,
        (sds((2 * LIST, 128)), slab, slab),
        [(v, VM) for v in (own, lists, xm, xp)],
        "yslab",
    )
    ym, yp = hop(hi, "gy", 1), hop(lo, "gy", -1)
    return call(
        main_kernel,
        (sds((1, 1, NS)), sds((1, 1, 4608))),
        [(v, VM) for v in (own, lists, xm, xp, ym, yp, *ws, jnp.asarray(fperm(), BF16))],
        "pairs",
        [
            pltpu.VMEM((64, PAIRS), F32), pltpu.VMEM((3, 64, PAIRS), F32),
            pltpu.VMEM((192, PAIRS), F32), pltpu.VMEM((9, 64, 128), F32),
            pltpu.VMEM((16, PAIRS), F32), pltpu.VMEM((64, PAIRS), F32),
            pltpu.VMEM((8, PAIRS + 128), F32), pltpu.VMEM((384, 256), BF16),
            pltpu.VMEM((80, 768), BF16), pltpu.VMEM((8, 128), F32),
            pltpu.VMEM((64, 128), F32), pltpu.VMEM((64, 128), F32),
        ],
        mib=16,
    )


def solution(mesh):
    cut = P("gx", "gy", "gz")
    return jax.shard_map(
        local,
        mesh=mesh,
        in_specs=(cut,) * 6 + (P(),) * 5,
        out_specs=(cut, cut),
        check_vma=False,
    )
```

```python
import math

import jax
import jax.numpy as jnp
import numpy as np
from jax import lax
from jax.experimental import pallas as pl
from jax.experimental.pallas import tpu as pltpu
from jax.sharding import PartitionSpec as P

F32 = jnp.float32
BF16 = jnp.bfloat16
CELL = 3.1
CUT = 6.0
VM = pl.BlockSpec(memory_space=pltpu.VMEM)
SM = pl.BlockSpec(memory_space=pltpu.SMEM)
HB = pl.BlockSpec(memory_space=pltpu.HBM)
PAIRS = 512
NS = 16
LIST = 40


def call(kernel, outs, ins, name, scratch=(), flops=0, mib=2):
    specs = [s for _, s in ins]
    return pl.pallas_call(
        kernel,
        out_shape=outs,
        in_specs=specs,
        out_specs=jax.tree.map(lambda _: VM, outs),
        scratch_shapes=list(scratch),
        name=name,
        compiler_params=pltpu.CompilerParams(vmem_limit_bytes=mib << 20),
        cost_estimate=pl.CostEstimate(flops=flops, bytes_accessed=0, transcendentals=0),
    )(*[a for a, _ in ins])


def split(v, parts):
    out = []
    for _ in range(parts - 1):
        h = v.astype(BF16)
        out.append(h)
        v = v - h.astype(F32)
    out.append(v.astype(BF16))
    return out


def mm(a, b, dims=((1,), (0,))):
    return lax.dot_general(a, b, (dims, ((), ())), preferred_element_type=F32)


def pack_kernel(d_in, s_in, nb_in, ce_in, ct_in, al_ref, o_ref, t_ref, d_ref, s_ref, nb_ref, ce_ref, ct_ref, sem):
    refs = (d_ref, s_ref, nb_ref, ce_ref, ct_ref)
    copies = [
        pltpu.make_async_copy(a, b, sem.at[i])
        for i, (a, b) in enumerate(zip((d_in, s_in, nb_in, ce_in, ct_in), refs))
    ]
    for c in copies:
        c.start()
    o_ref[48 : 48 + LIST, :] = jnp.zeros((LIST, 128), F32)
    t_ref[...] = jnp.zeros((128, 128), F32)
    for c in copies:
        c.wait()
    for i in range(36):
        o_ref[i : i + 1, :] = d_ref[0, :, 128 * i : 128 * i + 128]
    for i in range(12):
        o_ref[36 + i : 37 + i, :] = s_ref[0, :, 128 * i : 128 * i + 128].astype(F32)
    for i in range(4):
        v = nb_ref[0, :, 128 * i : 128 * i + 128].astype(F32)
        for c in range(4):
            t_ref[4 * i + c : 4 * i + c + 1, :] = pltpu.roll(v, (128 - 32 * c) % 128, axis=1)
    o_ref[48:80, 0:NS] = t_ref[...].T[0:32, 0:NS]
    lane = lax.broadcasted_iota(jnp.int32, (1, NS), 1)
    o_ref[80:81, 0:NS] = ce_ref[0].astype(F32)
    o_ref[81:82, 0:NS] = jnp.where(lane < al_ref[0], ct_ref[0], 0).astype(F32)


def zperm():
    m = np.zeros((3, 128, 256), np.float32)
    for s in range(16):
        d, z = (1, s + 4) if s < 4 else ((0, s - 4) if s < 12 else (2, s - 12))
        for a in range(3):
            at = (s // 8) * 128 + (s % 8) * 12 + a * 4
            for c in range(3):
                m[d, z * 9 + a * 3 + c, at + c] = 1.0
            m[d, 72 + z * 3 + a, at + 3] = 1.0
    return m.reshape(384, 256)


def zrows_kernel(e_ref, g_ref, p_ref, o_ref, l_ref, lo_ref, hi_ref, t_ref):
    e = e_ref[0]
    lane = lax.broadcasted_iota(jnp.int32, (4, 128), 1)
    wide = lax.broadcasted_iota(jnp.int32, (LIST, 128), 1)
    lists = jnp.zeros((LIST, 128), F32)
    for d in range(3):
        at = lax.rem(e + (0, 3, 1)[d], 4)
        for j in range(16):
            r, off = divmod(72 * j, 128)
            v = g_ref[at, pl.ds(r, 4, stride=9), :]
            v = pltpu.roll(v, (128 - off) % 128, axis=1) if off else v
            if off + 72 > 128:
                n = g_ref[at, pl.ds(r + 1, 4, stride=9), :]
                n = pltpu.roll(n, 128 - off, axis=1)
                v = jnp.where(lane < 128 - off, v, n)
            r, off = divmod(24 * j, 128)
            k = g_ref[at, pl.ds(36 + r, 4, stride=3), :]
            k = pltpu.roll(k, (72 - off) % 128, axis=1)
            if off + 24 > 128:
                n = g_ref[at, pl.ds(37 + r, 4, stride=3), :]
                n = pltpu.roll(n, (72 - off) % 128, axis=1)
                k = jnp.where(lane < 72 + 128 - off, k, n)
            v = jnp.where(lane < 72, v, jnp.where(lane < 96, k, 0.0))
            t_ref[d, pl.ds(j, 4, stride=16), :] = v
        b = NS * (1, 0, 2)[d]
        v = g_ref[at, 48 : 48 + LIST, :]
        v = pltpu.roll(v, b, axis=1) if b else v
        lists = jnp.where((wide >= b) & (wide < b + NS), v, lists)
    rows = jnp.concatenate([t_ref[0], t_ref[1], t_ref[2]], axis=1)
    r = mm(jnp.concatenate(split(rows, 3), axis=0), p_ref[...])
    r = (r[0:64] + r[64:128]) + r[128:192]
    l_ref[...] = lists
    for h in range(2):
        v = r[:, 128 * h : 128 * h + 128]
        o_ref[h] = v
        lo_ref[32 * h : 32 * h + 32, :] = v[0:32]
        hi_ref[32 * h : 32 * h + 32, :] = v[32:64]
    lo_ref[64 : 64 + LIST, :] = lists
    hi_ref[64 : 64 + LIST, :] = lists


def yslab_kernel(o_ref, l_ref, m_ref, p_ref, la_ref, lo_ref, hi_ref):
    lane = lax.broadcasted_iota(jnp.int32, (LIST, 128), 1)
    first = jnp.where(lane < 48, l_ref[...], pltpu.roll(m_ref[64 : 64 + LIST, :], 48, axis=1))
    second = p_ref[64 : 64 + LIST, :]
    la_ref[0:LIST, :] = first
    la_ref[LIST : 2 * LIST, :] = second
    for out, base in ((lo_ref, 0), (hi_ref, 4)):
        for h in range(2):
            for k in range(4):
                at = 64 * h + 16 * k
                out[at : at + 8, :] = o_ref[h, pl.ds(base + k, 8, stride=8), :]
                out[at + 8 : at + 12, :] = m_ref[pl.ds(32 * h + base + k, 4, stride=8), :]
                out[at + 12 : at + 16, :] = p_ref[pl.ds(32 * h + base + k, 4, stride=8), :]
        out[128 : 128 + LIST, :] = first
        out[128 + LIST : 128 + 2 * LIST, :] = second


def weights_kernel(w2, wl, we, wot, ro, t2, tl, te, to, bo, be, bl, b2, rc):
    def three(w):
        h, l = split(w, 2)
        return jnp.concatenate([h, h, l], axis=1)

    pad = jnp.concatenate([w2[...], jnp.zeros((4, 64), F32)], axis=0)
    t2[...] = three(pad.T)
    tl[...] = three(wl[...].T)
    te[...] = three(we[...].T)
    to[...] = three(wot[...])
    bo[...] = three(wot[...].T)
    be[...] = three(we[...])
    bl[...] = three(wl[...])
    b2[...] = three(w2[4:12, :])
    eye = lax.broadcasted_iota(jnp.int32, (64, 64), 0) == lax.broadcasted_iota(
        jnp.int32, (64, 64), 1
    )
    rc[...] = jnp.sum(jnp.where(eye, jnp.broadcast_to(ro[...], (64, 64)), 0.0), axis=1, keepdims=True)


def poly(x, coefs):
    acc = jnp.full_like(x, coefs[-1])
    for c in coefs[-2::-1]:
        acc = acc * x + c
    return acc


SIN = [math.pi ** (2 * k + 1) * (-1) ** k / math.factorial(2 * k + 1) for k in range(7)]
COS = [math.pi ** (2 * k) * (-1) ** k / math.factorial(2 * k) for k in range(8)]
R3, R5, R15 = math.sqrt(3.0), math.sqrt(5.0), math.sqrt(15.0)
ORDER = (0, 1, 1, 1, 2, 2, 2, 2, 2)


def stack3(v):
    h, l = split(v, 2)
    return jnp.concatenate([h, l, h], axis=0)


def quarter(v):
    return (v[:, 0:128] + v[:, 128:256]) + (v[:, 256:384] + v[:, 384:512])


def four(v):
    return jnp.concatenate([v] * 4, axis=1)


def div(v, k):
    return jnp.floor((v + 0.5) * (1.0 / k))


def cell_of(ce):
    cell = div(ce, 3)
    xy = div(cell, 8)
    x = div(xy, 8)
    return x, xy - 8.0 * x, cell - 8.0 * xy, ce - 3.0 * cell


def table_row(p, q):
    px = jnp.where(p < 4.0, p + 8.0, jnp.where(p < 12.0, p - 4.0, p))
    mid = q - 4.0 + 8.0 * jnp.where(p < 4.0, p + 8.0, jnp.where(p < 12.0, p - 4.0, p))
    return jnp.where(q < 4.0, 128.0 + 16.0 * q + px, jnp.where(q < 12.0, mid, 16.0 * q + px))


def place(x, y, z, atom):
    return (
        x + jnp.where(atom == 1.0, 0.75, 0.25),
        y + jnp.where(atom >= 1.0, 0.75, 0.25),
        z + jnp.where(atom == 2.0, 0.75, 0.25),
    )


def fperm():
    m = np.zeros((128, 128), np.float32)
    for z in range(8):
        for a in range(3):
            for c in range(3):
                m[z * 12 + a * 4 + c, z * 9 + a * 3 + c] = 1.0
    return m


def tiles(of):
    lane = lax.broadcasted_iota(jnp.int32, of, 1)
    row = lax.broadcasted_iota(jnp.int32, of, 0) if of[1] == 128 else lax.shift_right_logical(lane, 7)
    lane = lane & 127
    step = lax.shift_right_logical(row, 1)
    second = row & 1
    dy = jnp.where(step == 0, 0, jnp.where(step == 1, -1, 1))
    dx = jnp.where(second == 1, 1, jnp.where(lane < 48, 0, -1))
    at = jnp.where(lane < 48, lane, lane - 48)
    dz = lax.shift_right_logical(at, 4) - 1
    valid = (row < 6) & (lane < jnp.where(second == 1, 48, 96))
    return [v.astype(F32) for v in (dx, dy, dz)], valid, (row == 0) & (lane >= 16) & (lane < 32), lane


def main_kernel(
    o_ref, la_ref, xm_ref, xp_ref, ym_ref, yp_ref,
    t2, tl, te, to, bo, be, bl, b2, rc, fp_ref,
    en_ref, fo_ref,
    w_s, q_s, g_s, a_s, in_s, dw_s, sc_s, tb_s, ls_s, rk_s, acc_s, out_s, b_s,
):
    halves = []
    for h in range(2):
        v = jnp.concatenate(
            [
                o_ref[h], xm_ref[32 * h : 32 * h + 32, :], xp_ref[32 * h : 32 * h + 32, :],
                ym_ref[64 * h : 64 * h + 64, :], yp_ref[64 * h : 64 * h + 64, :],
            ],
            axis=0,
        )
        halves.append(v.T[0:96])
    tb_s[...] = jnp.concatenate(split(jnp.concatenate(halves, axis=0), 2), axis=0)

    places = [(la_ref, 0), (la_ref, LIST), (ym_ref, 128), (ym_ref, 128 + LIST), (yp_ref, 128), (yp_ref, 128 + LIST)]
    (dx, dy, dz), _, _, _ = tiles((1, 768))
    lst = jnp.concatenate([ref[at : at + LIST, :] for ref, at in places], axis=1)
    high = jnp.floor(lst[0:33] * (1.0 / 64.0))
    low = lst[0:33] - 64.0 * high
    ls_s[...] = jnp.concatenate(
        [
            high[0:32], low[0:32], high[32:33], low[32:33], lst[33:34],
            dx + 1.0, dy + 1.0, dz + 1.0, jnp.zeros((10, 768), F32),
        ],
        axis=0,
    ).astype(BF16)
    (dx, dy, dz), valid, own, lane = tiles((8, 128))
    pad = jnp.zeros((2, 128), F32)
    ce = jnp.concatenate([ref[at + 32 : at + 33, :] for ref, at in places] + [pad], axis=0)
    ct = jnp.concatenate([ref[at + 33 : at + 34, :] for ref, at in places] + [pad], axis=0)
    cx, cy, cz, _ = cell_of(ce)
    flag = valid & (~own) & (ct > 0.0)
    for c, d in ((cx, dx), (cy, dy), (cz, dz)):
        v = c + 8.0 * d
        flag = flag & (v >= -2.0) & (v < 10.0)
    flag = jnp.where(flag, 1.0, 0.0)
    tri = lax.broadcasted_iota(jnp.int32, (128, 128), 0) <= lax.broadcasted_iota(
        jnp.int32, (128, 128), 1
    )
    upto = mm(flag.astype(BF16), jnp.where(tri, 1.0, 0.0).astype(BF16))
    total = jnp.broadcast_to(jnp.sum(flag, axis=1, keepdims=True), (8, 128))
    row = lax.broadcasted_iota(jnp.int32, (8, 128), 0)
    before = jnp.where(row >= 1, pltpu.roll(total, 1, axis=0), 0.0)
    for by in (1, 2, 4):
        before = before + jnp.where(row >= by, pltpu.roll(before, by, axis=0), 0.0)
    rank = jnp.where(flag > 0.0, upto + before + (NS - 1.0), -1.0)
    rk_s[...] = jnp.where(own, (lane - 16).astype(F32), rank)
    ghosts = jnp.sum(flag).astype(jnp.int32)
    blocks = 1 + lax.shift_right_logical(ghosts + (NS - 1), 4)
    acc_s[...] = jnp.zeros((64, 128), F32)
    sc_s[...] = jnp.zeros((8, PAIRS + 128), F32)
    in_s[12:16, :] = jnp.zeros((4, PAIRS), F32)

    apart = lax.broadcasted_iota(jnp.int32, (128, 128), 0) - lax.broadcasted_iota(
        jnp.int32, (128, 128), 1
    )
    comb = jnp.where((apart & 15) == 0, 1.0, 0.0).astype(BF16)

    def slots_sum(v):
        r = mm(jnp.concatenate(split(v, 2), axis=0), comb)
        return r[0:576] + r[576:1152]

    def block(b, carry):
        want = (lax.broadcasted_iota(jnp.int32, (128, 128), 0) & 15) + NS * b
        want = want.astype(F32)
        chosen = jnp.concatenate(
            [jnp.where(want == rk_s[t : t + 1, :], 1.0, 0.0).astype(BF16) for t in range(6)], axis=1
        )
        u = mm(ls_s[...], chosen, ((1,), (1,)))
        sub = lax.broadcasted_iota(jnp.int32, (8, 128), 0)
        mine = sub == lax.shift_right_logical(lax.broadcasted_iota(jnp.int32, (8, 128), 1), 4)

        def slots(at):
            return jnp.concatenate(
                [
                    jnp.sum(jnp.where(mine, u[at + 8 * g : at + 8 * g + 8], 0.0), axis=0, keepdims=True)
                    for g in range(4)
                ],
                axis=1,
            )

        nb = 64.0 * slots(0) + slots(32)
        ce = 64.0 * u[64:65] + u[65:66]
        count = u[66:67]
        shift = [8.0 * (u[67 + k : 68 + k] - 1.0) for k in range(3)]
        cx, cy, cz, ca = cell_of(ce)
        cx, cy, cz = cx + shift[0], cy + shift[1], cz + shift[2]
        pq = div(nb, 36)
        r = nb - 36.0 * pq
        p = div(pq, 12)
        q = pq - 12.0 * p
        s = div(r, 3)
        a = r - 3.0 * s
        p = p + four(shift[0] - 2.0)
        q = q + four(shift[1] - 2.0)
        s = s + four(shift[2] - 2.0)
        lane = lax.broadcasted_iota(jnp.int32, (1, PAIRS), 1)
        alive = lax.shift_right_logical(lane, 4).astype(F32) < four(count)
        live = jnp.where(alive, 1.0, 0.0)
        second = place(p, q, s, a)
        centre = place(cx, cy, cz, ca)
        geo = [second[k] - four(centre[k]) for k in range(3)]
        rows = jnp.concatenate([table_row(p + 4.0, q + 4.0), table_row(cx + 4.0, cy + 4.0)], axis=1)
        rsel = jnp.concatenate([3.0 * (s + 4.0) + a, 3.0 * (cz + 4.0) + ca], axis=1)
        at = lax.broadcasted_iota(jnp.int32, (256, PAIRS + 128), 0).astype(F32)
        hot = jnp.where(at == rows, 1.0, 0.0).astype(BF16)

        got = mm(tb_s[...], hot)
        half = lax.shift_right_logical(
            lax.broadcasted_iota(jnp.int32, (8, PAIRS + 128), 0), 2
        ).astype(F32)
        pick = jnp.zeros((8, PAIRS + 128), F32)
        for k in range(24):
            v = got[8 * k : 8 * k + 8] + got[192 + 8 * k : 200 + 8 * k]
            pick = jnp.where(half + 2.0 * k == rsel, v, pick)
        pick = pick[0:4] + pick[4:8]
        first = four(pick[:, PAIRS:])
        second = pick[:, 0:PAIRS]
        rx = [
            jnp.where(alive, (geo[k] + (second[k : k + 1] - first[k : k + 1])) * CELL, 1.0)
            for k in range(3)
        ]
        d2 = rx[0] * rx[0] + rx[1] * rx[1] + rx[2] * rx[2]
        inv = lax.rsqrt(d2)
        inv = inv * (1.5 - 0.5 * d2 * inv * inv)
        dist = d2 * inv
        ux, uy, uz = [v * inv for v in rx]
        x = dist * (1.0 / CUT)
        inside = x < 1.0
        x = jnp.minimum(x, 1.0)
        x2 = x * x
        x3 = x2 * x
        x5 = x3 * x2
        x6 = x3 * x3
        env = jnp.where(inside, 1.0 + x6 * (-28.0 + x * (48.0 - 21.0 * x)), 0.0)
        denv_dd = jnp.where(inside, (-168.0 / CUT) * x5 * (1.0 - x) * (1.0 - x), 0.0)
        ev = env * live

        n = (lax.broadcasted_iota(jnp.int32, (8, PAIRS), 0) + 1).astype(F32)
        t = n * x
        k = jnp.floor(t + 0.5)
        f = t - k
        sign = 1.0 - 2.0 * (k - 2.0 * jnp.floor(k * 0.5))
        f2 = f * f
        sn = sign * f * poly(f2, SIN)
        cs = sign * poly(f2, COS)
        c0 = math.sqrt(2.0 / CUT)
        sd = sn * (c0 * inv)
        basis = sd * env
        dbasis = (n * cs) * ((c0 * math.pi / CUT) * inv * env) + sd * (denv_dd - env * inv)
        k1, k2 = first[3:4], second[3:4]
        in_s[0:1, :] = jnp.where(k1 == 0.0, 1.0, 0.0)
        in_s[1:2, :] = jnp.where(k1 == 1.0, 1.0, 0.0)
        in_s[2:3, :] = jnp.where(k2 == 0.0, 1.0, 0.0)
        in_s[3:4, :] = jnp.where(k2 == 1.0, 1.0, 0.0)
        in_s[4:12, :] = basis

        def silu(v):
            sg = 1.0 / (1.0 + jnp.exp(-v))
            return v * sg, sg * (1.0 + v * (1.0 - sg))

        h, dh_ = silu(mm(t2[...], stack3(in_s[...])))
        z, dz_ = silu(mm(tl[...], stack3(h)))
        zs = stack3(z)
        e = mm(te[...], zs)
        w_s[...] = e * ev

        ys = [
            None, R3 * ux, R3 * uy, R3 * uz, R15 * ux * uy, R15 * uy * uz,
            (0.5 * R5) * (3.0 * uz * uz - 1.0), R15 * ux * uz, (0.5 * R15) * (ux * ux - uy * uy),
        ]
        yb = [None] + [jnp.broadcast_to(v, (8, PAIRS)) for v in ys[1:]]
        for c in range(8):
            at = slice(8 * c, 8 * c + 8)
            w = w_s[at, :]
            for m in range(9):
                a_s[m, at, :] = 0.2 * quarter(w if m == 0 else w * yb[m])
        a_s[...] = slots_sum(a_s[...].reshape(576, 128)).reshape(9, 64, 128)
        for c in range(8):
            at = slice(8 * c, 8 * c + 8)
            sums = [None, None, None]
            for m in range(9):
                am = four(a_s[m, at, :])
                term = am if m == 0 else yb[m] * am
                l = ORDER[m]
                sums[l] = term if sums[l] is None else sums[l] + term
            for l in range(3):
                q_s[l, at, :] = sums[l]
        wv = w_s[...]
        joined = jnp.concatenate([z] + [wv * q_s[l] for l in range(3)], axis=0)
        y, dy_ = silu(mm(to[...], stack3(joined)))
        ro = rc[...]
        raw = jnp.sum(ro * y, axis=0, keepdims=True)

        @pl.when(b == 0)
        def _():
            en = quarter(raw * ev)
            for by in (16, 32, 64):
                en = en + pltpu.roll(en, by, axis=1)
            en_ref[...] = en[:, 0:NS].reshape(1, 1, NS)

        denv = live * raw
        dj = mm(bo[...], stack3((ro * ev) * dy_))
        g_s[...] = dj[64:256]
        for c in range(8):
            at = slice(8 * c, 8 * c + 8)
            w = w_s[at, :]
            for l in range(3):
                gw = g_s[64 * l + 8 * c : 64 * l + 8 * c + 8, :] * w
                for m in range(9):
                    if ORDER[m] == l:
                        b_s[m, at, :] = 0.2 * quarter(gw if m == 0 else gw * yb[m])
        b_s[...] = slots_sum(b_s[...].reshape(576, 128)).reshape(9, 64, 128)
        acc = [None] * 9
        for c in range(8):
            at = slice(8 * c, 8 * c + 8)
            w = w_s[at, :]
            dw = None
            for l in range(3):
                g = g_s[64 * l + 8 * c : 64 * l + 8 * c + 8, :]
                part = g * q_s[l, at, :]
                dw = part if dw is None else dw + part
                gw = g * w
                for m in range(9):
                    if ORDER[m] != l:
                        continue
                    bm = four(b_s[m, at, :])
                    dw = dw + (bm if m == 0 else yb[m] * bm)
                    if m:
                        v = gw * four(a_s[m, at, :]) + w * bm
                        acc[m] = v if acc[m] is None else acc[m] + v
            dw_s[at, :] = dw
        dw = dw_s[...]
        denv = denv + live * jnp.sum(dw * e, axis=0, keepdims=True)
        dz = dj[0:64] + mm(be[...], stack3(dw * ev))
        dh = mm(bl[...], stack3(dz * dz_))
        db = mm(b2[...], stack3(dh * dh_))
        dd = denv * denv_dd + jnp.sum(db * dbasis, axis=0, keepdims=True)
        dy = [None] + [jnp.sum(acc[m], axis=0, keepdims=True) for m in range(1, 9)]
        du0 = R3 * dy[1] + R15 * (uy * dy[4] + uz * dy[7] + ux * dy[8])
        du1 = R3 * dy[2] + R15 * (ux * dy[4] + uz * dy[5] - uy * dy[8])
        du2 = R3 * dy[3] + R15 * (uy * dy[5] + ux * dy[7]) + (3.0 * R5) * uz * dy[6]
        along = ux * du0 + uy * du1 + uz * du2
        dd = dd - along * inv
        grad = [du0 * inv + ux * dd, du1 * inv + uy * dd, du2 * inv + uz * dd]
        for k in range(3):
            mine = quarter(grad[k])
            for row in (k, k + 4):
                sc_s[row : row + 1, 0:PAIRS] = -grad[k]
                sc_s[row : row + 1, PAIRS:] = mine
        gv = sc_s[...]
        m = jnp.concatenate(
            [jnp.where(half + (12.0 + 2.0 * k) == rsel, gv, 0.0) for k in range(12)]
            + [jnp.zeros((32, PAIRS + 128), F32)],
            axis=0,
        )
        mh, ml = split(m, 2)
        nt = ((1,), (1,))
        acc_s[...] += mm(hot[0:64], mh, nt) + mm(hot[0:64], ml, nt)
        return carry

    lax.fori_loop(0, blocks, block, 0)

    r = mm(jnp.concatenate(split(acc_s[...], 3), axis=0), fp_ref[...])
    out_s[...] = (r[0:64] + r[64:128]) + r[128:192]
    lane = lax.broadcasted_iota(jnp.int32, (4, 128), 1)
    for k in range(9):
        v = jnp.zeros((4, 128), F32)
        for j in range(128 * k // 72, (128 * k + 127) // 72 + 1):
            off = 72 * j - 128 * k
            part = pltpu.roll(out_s[pl.ds(j, 4, stride=16), :], off % 128, axis=1)
            v = v + jnp.where((lane >= off) & (lane < off + 72), part, 0.0)
        for g in range(4):
            fo_ref[0, :, 128 * (9 * g + k) : 128 * (9 * g + k) + 128] = v[g : g + 1]


def sds(shape, dtype=F32):
    return jax.ShapeDtypeStruct(shape, dtype)


def hop(v, axis, by):
    n = lax.axis_size(axis)
    return lax.ppermute(v, axis, [(i, (i + by) % n) for i in range(n)])


def local(
    displacement, species, centres, neighbours, neighbour_count, live_centres,
    w_two, w_lat, w_env, w_out, readout,
):
    e = lax.axis_index("gz").astype(jnp.int32).reshape(1)
    flat = call(
        pack_kernel,
        sds((48 + LIST, 128)),
        [
            (pltpu.with_memory_space_constraint(v, pltpu.HBM), HB)
            for v in (displacement, species, neighbours, centres, neighbour_count)
        ]
        + [(live_centres.reshape(1), SM)],
        "pack",
        [
            pltpu.VMEM((128, 128), F32), pltpu.VMEM((1, 1, 4608), F32),
            pltpu.VMEM((1, 1, 1536), jnp.int32), pltpu.VMEM((1, 1, 512), jnp.int32),
            pltpu.VMEM((1, 1, NS), jnp.int32), pltpu.VMEM((1, 1, NS), jnp.int32),
            pltpu.SemaphoreType.DMA((5,)),
        ],
    )
    column = lax.all_gather(flat, "gz")
    slab = sds((64 + LIST, 128))
    own, lists, lo, hi = call(
        zrows_kernel,
        (sds((2, 64, 128)), sds((LIST, 128)), slab, slab),
        [(e, SM), (column, VM), (jnp.asarray(zperm(), BF16), VM)],
        "zrows",
        [pltpu.VMEM((3, 64, 128), F32)],
    )
    xm, xp = hop(hi, "gx", 1), hop(lo, "gx", -1)
    ws = call(
        weights_kernel,
        (
            sds((64, 48), BF16), sds((64, 192), BF16), sds((64, 192), BF16), sds((64, 768), BF16),
            sds((256, 192), BF16), sds((64, 192), BF16), sds((64, 192), BF16), sds((8, 192), BF16),
            sds((64, 1)),
        ),
        [(v, VM) for v in (w_two, w_lat, w_env, w_out.T, readout.reshape(1, 64))],
        "weights",
    )
    slab = sds((128 + 2 * LIST, 128))
    lists, lo, hi = call(
        yslab_kernel,
        (sds((2 * LIST, 128)), slab, slab),
        [(v, VM) for v in (own, lists, xm, xp)],
        "yslab",
    )
    ym, yp = hop(hi, "gy", 1), hop(lo, "gy", -1)
    return call(
        main_kernel,
        (sds((1, 1, NS)), sds((1, 1, 4608))),
        [(v, VM) for v in (own, lists, xm, xp, ym, yp, *ws, jnp.asarray(fperm(), BF16))],
        "pairs",
        [
            pltpu.VMEM((64, PAIRS), F32), pltpu.VMEM((3, 64, PAIRS), F32),
            pltpu.VMEM((192, PAIRS), F32), pltpu.VMEM((9, 64, 128), F32),
            pltpu.VMEM((16, PAIRS), F32), pltpu.VMEM((64, PAIRS), F32),
            pltpu.VMEM((8, PAIRS + 128), F32), pltpu.VMEM((384, 256), BF16),
            pltpu.VMEM((80, 768), BF16), pltpu.VMEM((8, 128), F32),
            pltpu.VMEM((64, 128), F32), pltpu.VMEM((64, 128), F32),
            pltpu.VMEM((9, 64, 128), F32),
        ],
        mib=16,
    )


def solution(mesh):
    cut = P("gx", "gy", "gz")
    return jax.shard_map(
        local,
        mesh=mesh,
        in_specs=(cut,) * 6 + (P(),) * 5,
        out_specs=(cut, cut),
        check_vma=False,
    )
```

```python
import math

import jax
import jax.numpy as jnp
import numpy as np
from jax import lax
from jax.experimental import pallas as pl
from jax.experimental.pallas import tpu as pltpu
from jax.sharding import PartitionSpec as P

F32 = jnp.float32
BF16 = jnp.bfloat16
CELL = 3.1
CUT = 6.0
VM = pl.BlockSpec(memory_space=pltpu.VMEM)
SM = pl.BlockSpec(memory_space=pltpu.SMEM)
HB = pl.BlockSpec(memory_space=pltpu.HBM)
NS = 16
NB = 64
PAIRS = 32 * NB
TILES = PAIRS // 128
LIST = 40


def call(kernel, outs, ins, name, scratch=(), flops=0, mib=2):
    specs = [s for _, s in ins]
    return pl.pallas_call(
        kernel,
        out_shape=outs,
        in_specs=specs,
        out_specs=jax.tree.map(lambda _: VM, outs),
        scratch_shapes=list(scratch),
        name=name,
        compiler_params=pltpu.CompilerParams(vmem_limit_bytes=mib << 20),
        cost_estimate=pl.CostEstimate(flops=flops, bytes_accessed=0, transcendentals=0),
    )(*[a for a, _ in ins])


def split(v, parts):
    out = []
    for _ in range(parts - 1):
        h = v.astype(BF16)
        out.append(h)
        v = v - h.astype(F32)
    out.append(v.astype(BF16))
    return out


def mm(a, b, dims=((1,), (0,))):
    return lax.dot_general(a, b, (dims, ((), ())), preferred_element_type=F32)


def pack_kernel(d_in, s_in, nb_in, ce_in, ct_in, al_ref, o_ref, t_ref, d_ref, s_ref, nb_ref, ce_ref, ct_ref, sem):
    refs = (d_ref, s_ref, nb_ref, ce_ref, ct_ref)
    copies = [
        pltpu.make_async_copy(a, b, sem.at[i])
        for i, (a, b) in enumerate(zip((d_in, s_in, nb_in, ce_in, ct_in), refs))
    ]
    for c in copies:
        c.start()
    o_ref[48 : 48 + LIST, :] = jnp.zeros((LIST, 128), F32)
    t_ref[...] = jnp.zeros((128, 128), F32)
    for c in copies:
        c.wait()
    for i in range(36):
        o_ref[i : i + 1, :] = d_ref[0, :, 128 * i : 128 * i + 128]
    for i in range(12):
        o_ref[36 + i : 37 + i, :] = s_ref[0, :, 128 * i : 128 * i + 128].astype(F32)
    for i in range(4):
        v = nb_ref[0, :, 128 * i : 128 * i + 128].astype(F32)
        for c in range(4):
            t_ref[4 * i + c : 4 * i + c + 1, :] = pltpu.roll(v, (128 - 32 * c) % 128, axis=1)
    o_ref[48:80, 0:NS] = t_ref[...].T[0:32, 0:NS]
    lane = lax.broadcasted_iota(jnp.int32, (1, NS), 1)
    o_ref[80:81, 0:NS] = ce_ref[0].astype(F32)
    o_ref[81:82, 0:NS] = jnp.where(lane < al_ref[0], ct_ref[0], 0).astype(F32)


def zperm():
    m = np.zeros((3, 128, 256), np.float32)
    for s in range(16):
        d, z = (1, s + 4) if s < 4 else ((0, s - 4) if s < 12 else (2, s - 12))
        for a in range(3):
            at = (s // 8) * 128 + (s % 8) * 12 + a * 4
            for c in range(3):
                m[d, z * 9 + a * 3 + c, at + c] = 1.0
            m[d, 72 + z * 3 + a, at + 3] = 1.0
    return m.reshape(384, 256)


def zrows_kernel(e_ref, g_ref, p_ref, o_ref, l_ref, lo_ref, hi_ref, t_ref):
    e = e_ref[0]
    lane = lax.broadcasted_iota(jnp.int32, (4, 128), 1)
    wide = lax.broadcasted_iota(jnp.int32, (LIST, 128), 1)
    lists = jnp.zeros((LIST, 128), F32)
    for d in range(3):
        at = lax.rem(e + (0, 3, 1)[d], 4)
        for j in range(16):
            r, off = divmod(72 * j, 128)
            v = g_ref[at, pl.ds(r, 4, stride=9), :]
            v = pltpu.roll(v, (128 - off) % 128, axis=1) if off else v
            if off + 72 > 128:
                n = g_ref[at, pl.ds(r + 1, 4, stride=9), :]
                n = pltpu.roll(n, 128 - off, axis=1)
                v = jnp.where(lane < 128 - off, v, n)
            r, off = divmod(24 * j, 128)
            k = g_ref[at, pl.ds(36 + r, 4, stride=3), :]
            k = pltpu.roll(k, (72 - off) % 128, axis=1)
            if off + 24 > 128:
                n = g_ref[at, pl.ds(37 + r, 4, stride=3), :]
                n = pltpu.roll(n, (72 - off) % 128, axis=1)
                k = jnp.where(lane < 72 + 128 - off, k, n)
            v = jnp.where(lane < 72, v, jnp.where(lane < 96, k, 0.0))
            t_ref[d, pl.ds(j, 4, stride=16), :] = v
        b = NS * (1, 0, 2)[d]
        v = g_ref[at, 48 : 48 + LIST, :]
        v = pltpu.roll(v, b, axis=1) if b else v
        lists = jnp.where((wide >= b) & (wide < b + NS), v, lists)
    rows = jnp.concatenate([t_ref[0], t_ref[1], t_ref[2]], axis=1)
    r = mm(jnp.concatenate(split(rows, 3), axis=0), p_ref[...])
    r = (r[0:64] + r[64:128]) + r[128:192]
    l_ref[...] = lists
    for h in range(2):
        v = r[:, 128 * h : 128 * h + 128]
        o_ref[h] = v
        lo_ref[32 * h : 32 * h + 32, :] = v[0:32]
        hi_ref[32 * h : 32 * h + 32, :] = v[32:64]
    lo_ref[64 : 64 + LIST, :] = lists
    hi_ref[64 : 64 + LIST, :] = lists


def yslab_kernel(o_ref, l_ref, m_ref, p_ref, la_ref, lo_ref, hi_ref):
    lane = lax.broadcasted_iota(jnp.int32, (LIST, 128), 1)
    first = jnp.where(lane < 48, l_ref[...], pltpu.roll(m_ref[64 : 64 + LIST, :], 48, axis=1))
    second = p_ref[64 : 64 + LIST, :]
    la_ref[0:LIST, :] = first
    la_ref[LIST : 2 * LIST, :] = second
    for out, base in ((lo_ref, 0), (hi_ref, 4)):
        for h in range(2):
            for k in range(4):
                at = 64 * h + 16 * k
                out[at : at + 8, :] = o_ref[h, pl.ds(base + k, 8, stride=8), :]
                out[at + 8 : at + 12, :] = m_ref[pl.ds(32 * h + base + k, 4, stride=8), :]
                out[at + 12 : at + 16, :] = p_ref[pl.ds(32 * h + base + k, 4, stride=8), :]
        out[128 : 128 + LIST, :] = first
        out[128 + LIST : 128 + 2 * LIST, :] = second


def weights_kernel(w2, wl, we, wot, ro, t2, tl, te, to, bo, be, bl, b2, rc):
    def three(w):
        h, l = split(w, 2)
        return jnp.concatenate([h, h, l], axis=1)

    pad = jnp.concatenate([w2[...], jnp.zeros((4, 64), F32)], axis=0)
    t2[...] = three(pad.T)
    tl[...] = three(wl[...].T)
    te[...] = three(we[...].T)
    to[...] = three(wot[...])
    bo[...] = three(wot[...].T)
    be[...] = three(we[...])
    bl[...] = three(wl[...])
    b2[...] = three(w2[4:12, :])
    eye = lax.broadcasted_iota(jnp.int32, (64, 64), 0) == lax.broadcasted_iota(
        jnp.int32, (64, 64), 1
    )
    rc[...] = jnp.sum(jnp.where(eye, jnp.broadcast_to(ro[...], (64, 64)), 0.0), axis=1, keepdims=True)


def poly(x, coefs):
    acc = jnp.full_like(x, coefs[-1])
    for c in coefs[-2::-1]:
        acc = acc * x + c
    return acc


SIN = [math.pi ** (2 * k + 1) * (-1) ** k / math.factorial(2 * k + 1) for k in range(7)]
COS = [math.pi ** (2 * k) * (-1) ** k / math.factorial(2 * k) for k in range(8)]
R3, R5, R15 = math.sqrt(3.0), math.sqrt(5.0), math.sqrt(15.0)
ORDER = (0, 1, 1, 1, 2, 2, 2, 2, 2)


def stack3(v):
    h, l = split(v, 2)
    return jnp.concatenate([h, l, h], axis=0)


def fold(v):
    parts = [v[:, 128 * i : 128 * i + 128] for i in range(TILES)]
    while len(parts) > 1:
        parts = [a + b for a, b in zip(parts[0::2], parts[1::2])]
    return parts[0]


def wide(v):
    return jnp.concatenate([v] * TILES, axis=1)


def div(v, k):
    return jnp.floor((v + 0.5) * (1.0 / k))


def cell_of(ce):
    cell = div(ce, 3)
    xy = div(cell, 8)
    x = div(xy, 8)
    return x, xy - 8.0 * x, cell - 8.0 * xy, ce - 3.0 * cell


def table_row(p, q):
    px = jnp.where(p < 4.0, p + 8.0, jnp.where(p < 12.0, p - 4.0, p))
    mid = q - 4.0 + 8.0 * jnp.where(p < 4.0, p + 8.0, jnp.where(p < 12.0, p - 4.0, p))
    return jnp.where(q < 4.0, 128.0 + 16.0 * q + px, jnp.where(q < 12.0, mid, 16.0 * q + px))


def place(x, y, z, atom):
    return (
        x + jnp.where(atom == 1.0, 0.75, 0.25),
        y + jnp.where(atom >= 1.0, 0.75, 0.25),
        z + jnp.where(atom == 2.0, 0.75, 0.25),
    )


def fperm():
    m = np.zeros((128, 128), np.float32)
    for z in range(8):
        for a in range(3):
            for c in range(3):
                m[z * 12 + a * 4 + c, z * 9 + a * 3 + c] = 1.0
    return m


def tiles(of):
    lane = lax.broadcasted_iota(jnp.int32, of, 1)
    row = lax.broadcasted_iota(jnp.int32, of, 0) if of[1] == 128 else lax.shift_right_logical(lane, 7)
    lane = lane & 127
    step = lax.shift_right_logical(row, 1)
    second = row & 1
    dy = jnp.where(step == 0, 0, jnp.where(step == 1, -1, 1))
    dx = jnp.where(second == 1, 1, jnp.where(lane < 48, 0, -1))
    at = jnp.where(lane < 48, lane, lane - 48)
    dz = lax.shift_right_logical(at, 4) - 1
    valid = (row < 6) & (lane < jnp.where(second == 1, 48, 96))
    return [v.astype(F32) for v in (dx, dy, dz)], valid, (row == 0) & (lane >= 16) & (lane < 32), lane


def main_kernel(
    o_ref, la_ref, xm_ref, xp_ref, ym_ref, yp_ref,
    t2, tl, te, to, bo, be, bl, b2, rc, fp_ref,
    en_ref, fo_ref,
    w_s, q_s, g_s, a_s, in_s, dw_s, sc_s, tb_s, ls_s, rk_s, acc_s, out_s, b_s,
):
    halves = []
    for h in range(2):
        v = jnp.concatenate(
            [
                o_ref[h], xm_ref[32 * h : 32 * h + 32, :], xp_ref[32 * h : 32 * h + 32, :],
                ym_ref[64 * h : 64 * h + 64, :], yp_ref[64 * h : 64 * h + 64, :],
            ],
            axis=0,
        )
        halves.append(v.T[0:96])
    tb_s[...] = jnp.concatenate(split(jnp.concatenate(halves, axis=0), 2), axis=0)

    places = [(la_ref, 0), (la_ref, LIST), (ym_ref, 128), (ym_ref, 128 + LIST), (yp_ref, 128), (yp_ref, 128 + LIST)]
    (dx, dy, dz), _, _, _ = tiles((1, 768))
    lst = jnp.concatenate([ref[at : at + LIST, :] for ref, at in places], axis=1)
    high = jnp.floor(lst[0:33] * (1.0 / 64.0))
    low = lst[0:33] - 64.0 * high
    ls_s[...] = jnp.concatenate(
        [
            high[0:32], low[0:32], high[32:33], low[32:33], lst[33:34],
            dx + 1.0, dy + 1.0, dz + 1.0, jnp.zeros((10, 768), F32),
        ],
        axis=0,
    ).astype(BF16)
    (dx, dy, dz), valid, own, lane = tiles((8, 128))
    pad = jnp.zeros((2, 128), F32)
    ce = jnp.concatenate([ref[at + 32 : at + 33, :] for ref, at in places] + [pad], axis=0)
    ct = jnp.concatenate([ref[at + 33 : at + 34, :] for ref, at in places] + [pad], axis=0)
    cx, cy, cz, _ = cell_of(ce)
    flag = valid & (~own) & (ct > 0.0)
    for c, d in ((cx, dx), (cy, dy), (cz, dz)):
        v = c + 8.0 * d
        flag = flag & (v >= -2.0) & (v < 10.0)
    flag = jnp.where(flag, 1.0, 0.0)
    tri = lax.broadcasted_iota(jnp.int32, (128, 128), 0) <= lax.broadcasted_iota(
        jnp.int32, (128, 128), 1
    )
    upto = mm(flag.astype(BF16), jnp.where(tri, 1.0, 0.0).astype(BF16))
    total = jnp.broadcast_to(jnp.sum(flag, axis=1, keepdims=True), (8, 128))
    row = lax.broadcasted_iota(jnp.int32, (8, 128), 0)
    before = jnp.where(row >= 1, pltpu.roll(total, 1, axis=0), 0.0)
    for by in (1, 2, 4):
        before = before + jnp.where(row >= by, pltpu.roll(before, by, axis=0), 0.0)
    mine = own & (ct > 0.0)
    owned = jnp.sum(jnp.where(mine, 1.0, 0.0))
    rank = jnp.where(flag > 0.0, upto + before + (owned - 1.0), -1.0)
    rk_s[...] = jnp.where(mine, (lane - 16).astype(F32), rank)
    blocks = lax.div((owned + jnp.sum(flag)).astype(jnp.int32) + (NB - 1), NB)
    acc_s[...] = jnp.zeros((64, 128), F32)
    sc_s[...] = jnp.zeros((8, PAIRS + 128), F32)
    in_s[12:16, :] = jnp.zeros((4, PAIRS), F32)

    apart = lax.broadcasted_iota(jnp.int32, (128, 128), 0) - lax.broadcasted_iota(
        jnp.int32, (128, 128), 1
    )
    comb = jnp.where((apart & (NB - 1)) == 0, 1.0, 0.0).astype(BF16)

    def slots_sum(v):
        r = mm(jnp.concatenate(split(v, 2), axis=0), comb)
        return r[0:576] + r[576:1152]

    def block(b, carry):
        want = (lax.broadcasted_iota(jnp.int32, (128, 128), 0) & (NB - 1)) + NB * b
        want = want.astype(F32)
        chosen = jnp.concatenate(
            [jnp.where(want == rk_s[t : t + 1, :], 1.0, 0.0).astype(BF16) for t in range(6)], axis=1
        )
        u = mm(ls_s[...], chosen, ((1,), (1,)))
        left = lax.broadcasted_iota(jnp.int32, (1, 128), 1) < NB

        def slots(at):
            return jnp.concatenate(
                [
                    jnp.where(left, u[at + 2 * g : at + 2 * g + 1], u[at + 2 * g + 1 : at + 2 * g + 2])
                    for g in range(TILES)
                ],
                axis=1,
            )

        nb = 64.0 * slots(0) + slots(32)
        ce = 64.0 * u[64:65] + u[65:66]
        count = u[66:67]
        shift = [8.0 * (u[67 + k : 68 + k] - 1.0) for k in range(3)]
        cx, cy, cz, ca = cell_of(ce)
        cx, cy, cz = cx + shift[0], cy + shift[1], cz + shift[2]
        pq = div(nb, 36)
        r = nb - 36.0 * pq
        p = div(pq, 12)
        q = pq - 12.0 * p
        s = div(r, 3)
        a = r - 3.0 * s
        p = p + wide(shift[0] - 2.0)
        q = q + wide(shift[1] - 2.0)
        s = s + wide(shift[2] - 2.0)
        lane = lax.broadcasted_iota(jnp.int32, (1, PAIRS), 1)
        alive = lax.div(lane, NB).astype(F32) < wide(count)
        live = jnp.where(alive, 1.0, 0.0)
        second = place(p, q, s, a)
        centre = place(cx, cy, cz, ca)
        geo = [second[k] - wide(centre[k]) for k in range(3)]
        rows = jnp.concatenate([table_row(p + 4.0, q + 4.0), table_row(cx + 4.0, cy + 4.0)], axis=1)
        rsel = jnp.concatenate([3.0 * (s + 4.0) + a, 3.0 * (cz + 4.0) + ca], axis=1)
        at = lax.broadcasted_iota(jnp.int32, (256, PAIRS + 128), 0).astype(F32)
        hot = jnp.where(at == rows, 1.0, 0.0).astype(BF16)

        got = mm(tb_s[...], hot)
        half = lax.shift_right_logical(
            lax.broadcasted_iota(jnp.int32, (8, PAIRS + 128), 0), 2
        ).astype(F32)
        pick = jnp.zeros((8, PAIRS + 128), F32)
        for k in range(24):
            v = got[8 * k : 8 * k + 8] + got[192 + 8 * k : 200 + 8 * k]
            pick = jnp.where(half + 2.0 * k == rsel, v, pick)
        pick = pick[0:4] + pick[4:8]
        first = wide(pick[:, PAIRS:])
        second = pick[:, 0:PAIRS]
        rx = [
            jnp.where(alive, (geo[k] + (second[k : k + 1] - first[k : k + 1])) * CELL, 1.0)
            for k in range(3)
        ]
        d2 = rx[0] * rx[0] + rx[1] * rx[1] + rx[2] * rx[2]
        inv = lax.rsqrt(d2)
        inv = inv * (1.5 - 0.5 * d2 * inv * inv)
        dist = d2 * inv
        ux, uy, uz = [v * inv for v in rx]
        x = dist * (1.0 / CUT)
        inside = x < 1.0
        x = jnp.minimum(x, 1.0)
        x2 = x * x
        x3 = x2 * x
        x5 = x3 * x2
        x6 = x3 * x3
        env = jnp.where(inside, 1.0 + x6 * (-28.0 + x * (48.0 - 21.0 * x)), 0.0)
        denv_dd = jnp.where(inside, (-168.0 / CUT) * x5 * (1.0 - x) * (1.0 - x), 0.0)
        ev = env * live

        n = (lax.broadcasted_iota(jnp.int32, (8, PAIRS), 0) + 1).astype(F32)
        t = n * x
        k = jnp.floor(t + 0.5)
        f = t - k
        sign = 1.0 - 2.0 * (k - 2.0 * jnp.floor(k * 0.5))
        f2 = f * f
        sn = sign * f * poly(f2, SIN)
        cs = sign * poly(f2, COS)
        c0 = math.sqrt(2.0 / CUT)
        sd = sn * (c0 * inv)
        basis = sd * env
        dbasis = (n * cs) * ((c0 * math.pi / CUT) * inv * env) + sd * (denv_dd - env * inv)
        k1, k2 = first[3:4], second[3:4]
        in_s[0:1, :] = jnp.where(k1 == 0.0, 1.0, 0.0)
        in_s[1:2, :] = jnp.where(k1 == 1.0, 1.0, 0.0)
        in_s[2:3, :] = jnp.where(k2 == 0.0, 1.0, 0.0)
        in_s[3:4, :] = jnp.where(k2 == 1.0, 1.0, 0.0)
        in_s[4:12, :] = basis

        def silu(v):
            sg = 0.5 + 0.5 * jnp.tanh(0.5 * v)
            return v * sg, sg * (1.0 + v * (1.0 - sg))

        h, dh_ = silu(mm(t2[...], stack3(in_s[...])))
        z, dz_ = silu(mm(tl[...], stack3(h)))
        zs = stack3(z)
        e = mm(te[...], zs)
        w_s[...] = e * ev

        ys = [
            None, R3 * ux, R3 * uy, R3 * uz, R15 * ux * uy, R15 * uy * uz,
            (0.5 * R5) * (3.0 * uz * uz - 1.0), R15 * ux * uz, (0.5 * R15) * (ux * ux - uy * uy),
        ]
        yb = [None] + [jnp.broadcast_to(v, (8, PAIRS)) for v in ys[1:]]
        for c in range(8):
            at = slice(8 * c, 8 * c + 8)
            w = w_s[at, :]
            for m in range(9):
                a_s[m, at, :] = 0.2 * fold(w if m == 0 else w * yb[m])
        a_s[...] = slots_sum(a_s[...].reshape(576, 128)).reshape(9, 64, 128)
        for c in range(8):
            at = slice(8 * c, 8 * c + 8)
            sums = [None, None, None]
            for m in range(9):
                am = wide(a_s[m, at, :])
                term = am if m == 0 else yb[m] * am
                l = ORDER[m]
                sums[l] = term if sums[l] is None else sums[l] + term
            for l in range(3):
                q_s[l, at, :] = sums[l]
        wv = w_s[...]
        joined = jnp.concatenate([z] + [wv * q_s[l] for l in range(3)], axis=0)
        y, dy_ = silu(mm(to[...], stack3(joined)))
        ro = rc[...]
        raw = jnp.sum(ro * y, axis=0, keepdims=True)

        @pl.when(b == 0)
        def _():
            en = fold(raw * ev)
            en = en + pltpu.roll(en, NB, axis=1)
            first_lanes = lax.broadcasted_iota(jnp.int32, (1, 128), 1).astype(F32)
            en = jnp.where(first_lanes < owned, en, 0.0)
            en_ref[...] = en[:, 0:NS].reshape(1, 1, NS)

        denv = live * raw
        dj = mm(bo[...], stack3((ro * ev) * dy_))
        g_s[...] = dj[64:256]
        for c in range(8):
            at = slice(8 * c, 8 * c + 8)
            w = w_s[at, :]
            for l in range(3):
                gw = g_s[64 * l + 8 * c : 64 * l + 8 * c + 8, :] * w
                for m in range(9):
                    if ORDER[m] == l:
                        b_s[m, at, :] = 0.2 * fold(gw if m == 0 else gw * yb[m])
        b_s[...] = slots_sum(b_s[...].reshape(576, 128)).reshape(9, 64, 128)
        acc = [None] * 9
        for c in range(8):
            at = slice(8 * c, 8 * c + 8)
            w = w_s[at, :]
            dw = None
            for l in range(3):
                g = g_s[64 * l + 8 * c : 64 * l + 8 * c + 8, :]
                part = g * q_s[l, at, :]
                dw = part if dw is None else dw + part
                gw = g * w
                for m in range(9):
                    if ORDER[m] != l:
                        continue
                    bm = wide(b_s[m, at, :])
                    dw = dw + (bm if m == 0 else yb[m] * bm)
                    if m:
                        v = gw * wide(a_s[m, at, :]) + w * bm
                        acc[m] = v if acc[m] is None else acc[m] + v
            dw_s[at, :] = dw
        dw = dw_s[...]
        denv = denv + live * jnp.sum(dw * e, axis=0, keepdims=True)
        dz = dj[0:64] + mm(be[...], stack3(dw * ev))
        dh = mm(bl[...], stack3(dz * dz_))
        db = mm(b2[...], stack3(dh * dh_))
        dd = denv * denv_dd + jnp.sum(db * dbasis, axis=0, keepdims=True)
        dy = [None] + [jnp.sum(acc[m], axis=0, keepdims=True) for m in range(1, 9)]
        du0 = R3 * dy[1] + R15 * (uy * dy[4] + uz * dy[7] + ux * dy[8])
        du1 = R3 * dy[2] + R15 * (ux * dy[4] + uz * dy[5] - uy * dy[8])
        du2 = R3 * dy[3] + R15 * (uy * dy[5] + ux * dy[7]) + (3.0 * R5) * uz * dy[6]
        along = ux * du0 + uy * du1 + uz * du2
        dd = dd - along * inv
        grad = [du0 * inv + ux * dd, du1 * inv + uy * dd, du2 * inv + uz * dd]
        for k in range(3):
            mine = fold(grad[k])
            for row in (k, k + 4):
                sc_s[row : row + 1, 0:PAIRS] = -grad[k]
                sc_s[row : row + 1, PAIRS:] = mine
        gv = sc_s[...]
        m = jnp.concatenate(
            [jnp.where(half + (12.0 + 2.0 * k) == rsel, gv, 0.0) for k in range(12)]
            + [jnp.zeros((32, PAIRS + 128), F32)],
            axis=0,
        )
        mh, ml = split(m, 2)
        nt = ((1,), (1,))
        acc_s[...] += mm(hot[0:64], mh, nt) + mm(hot[0:64], ml, nt)
        return carry

    lax.fori_loop(0, blocks, block, 0)

    r = mm(jnp.concatenate(split(acc_s[...], 3), axis=0), fp_ref[...])
    out_s[...] = (r[0:64] + r[64:128]) + r[128:192]
    lane = lax.broadcasted_iota(jnp.int32, (4, 128), 1)
    for k in range(9):
        v = jnp.zeros((4, 128), F32)
        for j in range(128 * k // 72, (128 * k + 127) // 72 + 1):
            off = 72 * j - 128 * k
            part = pltpu.roll(out_s[pl.ds(j, 4, stride=16), :], off % 128, axis=1)
            v = v + jnp.where((lane >= off) & (lane < off + 72), part, 0.0)
        for g in range(4):
            fo_ref[0, :, 128 * (9 * g + k) : 128 * (9 * g + k) + 128] = v[g : g + 1]


def sds(shape, dtype=F32):
    return jax.ShapeDtypeStruct(shape, dtype)


def hop(v, axis, by):
    n = lax.axis_size(axis)
    return lax.ppermute(v, axis, [(i, (i + by) % n) for i in range(n)])


def local(
    displacement, species, centres, neighbours, neighbour_count, live_centres,
    w_two, w_lat, w_env, w_out, readout,
):
    e = lax.axis_index("gz").astype(jnp.int32).reshape(1)
    flat = call(
        pack_kernel,
        sds((48 + LIST, 128)),
        [
            (pltpu.with_memory_space_constraint(v, pltpu.HBM), HB)
            for v in (displacement, species, neighbours, centres, neighbour_count)
        ]
        + [(live_centres.reshape(1), SM)],
        "pack",
        [
            pltpu.VMEM((128, 128), F32), pltpu.VMEM((1, 1, 4608), F32),
            pltpu.VMEM((1, 1, 1536), jnp.int32), pltpu.VMEM((1, 1, 512), jnp.int32),
            pltpu.VMEM((1, 1, NS), jnp.int32), pltpu.VMEM((1, 1, NS), jnp.int32),
            pltpu.SemaphoreType.DMA((5,)),
        ],
    )
    column = lax.all_gather(flat, "gz")
    slab = sds((64 + LIST, 128))
    own, lists, lo, hi = call(
        zrows_kernel,
        (sds((2, 64, 128)), sds((LIST, 128)), slab, slab),
        [(e, SM), (column, VM), (jnp.asarray(zperm(), BF16), VM)],
        "zrows",
        [pltpu.VMEM((3, 64, 128), F32)],
    )
    xm, xp = hop(hi, "gx", 1), hop(lo, "gx", -1)
    ws = call(
        weights_kernel,
        (
            sds((64, 48), BF16), sds((64, 192), BF16), sds((64, 192), BF16), sds((64, 768), BF16),
            sds((256, 192), BF16), sds((64, 192), BF16), sds((64, 192), BF16), sds((8, 192), BF16),
            sds((64, 1)),
        ),
        [(v, VM) for v in (w_two, w_lat, w_env, w_out.T, readout.reshape(1, 64))],
        "weights",
    )
    slab = sds((128 + 2 * LIST, 128))
    lists, lo, hi = call(
        yslab_kernel,
        (sds((2 * LIST, 128)), slab, slab),
        [(v, VM) for v in (own, lists, xm, xp)],
        "yslab",
    )
    ym, yp = hop(hi, "gy", 1), hop(lo, "gy", -1)
    return call(
        main_kernel,
        (sds((1, 1, NS)), sds((1, 1, 4608))),
        [(v, VM) for v in (own, lists, xm, xp, ym, yp, *ws, jnp.asarray(fperm(), BF16))],
        "pairs",
        [
            pltpu.VMEM((64, PAIRS), F32), pltpu.VMEM((3, 64, PAIRS), F32),
            pltpu.VMEM((192, PAIRS), F32), pltpu.VMEM((9, 64, 128), F32),
            pltpu.VMEM((16, PAIRS), F32), pltpu.VMEM((64, PAIRS), F32),
            pltpu.VMEM((8, PAIRS + 128), F32), pltpu.VMEM((384, 256), BF16),
            pltpu.VMEM((80, 768), BF16), pltpu.VMEM((8, 128), F32),
            pltpu.VMEM((64, 128), F32), pltpu.VMEM((64, 128), F32),
            pltpu.VMEM((9, 64, 128), F32),
        ],
        mib=24,
    )


def solution(mesh):
    cut = P("gx", "gy", "gz")
    return jax.shard_map(
        local,
        mesh=mesh,
        in_specs=(cut,) * 6 + (P(),) * 5,
        out_specs=(cut, cut),
        check_vma=False,
    )
```

```python
import math

import jax
import jax.numpy as jnp
import numpy as np
from jax import lax
from jax.experimental import pallas as pl
from jax.experimental.pallas import tpu as pltpu
from jax.sharding import PartitionSpec as P

F32 = jnp.float32
BF16 = jnp.bfloat16
CELL = 3.1
CUT = 6.0
VM = pl.BlockSpec(memory_space=pltpu.VMEM)
SM = pl.BlockSpec(memory_space=pltpu.SMEM)
HB = pl.BlockSpec(memory_space=pltpu.HBM)
NS = 16
TILES = 12
PAIRS = 128 * TILES
FULL = 42
LIST = 40


def call(kernel, outs, ins, name, scratch=(), flops=0, mib=2):
    specs = [s for _, s in ins]
    return pl.pallas_call(
        kernel,
        out_shape=outs,
        in_specs=specs,
        out_specs=jax.tree.map(lambda _: VM, outs),
        scratch_shapes=list(scratch),
        name=name,
        compiler_params=pltpu.CompilerParams(vmem_limit_bytes=mib << 20),
        cost_estimate=pl.CostEstimate(flops=flops, bytes_accessed=0, transcendentals=0),
    )(*[a for a, _ in ins])


def split(v, parts):
    out = []
    for _ in range(parts - 1):
        h = v.astype(BF16)
        out.append(h)
        v = v - h.astype(F32)
    out.append(v.astype(BF16))
    return out


def mm(a, b, dims=((1,), (0,))):
    return lax.dot_general(a, b, (dims, ((), ())), preferred_element_type=F32)


def pack_kernel(d_in, s_in, nb_in, ce_in, ct_in, al_ref, o_ref, t_ref, d_ref, s_ref, nb_ref, ce_ref, ct_ref, sem):
    refs = (d_ref, s_ref, nb_ref, ce_ref, ct_ref)
    copies = [
        pltpu.make_async_copy(a, b, sem.at[i])
        for i, (a, b) in enumerate(zip((d_in, s_in, nb_in, ce_in, ct_in), refs))
    ]
    for c in copies:
        c.start()
    o_ref[48 : 48 + LIST, :] = jnp.zeros((LIST, 128), F32)
    t_ref[...] = jnp.zeros((128, 128), F32)
    for c in copies:
        c.wait()
    for i in range(36):
        o_ref[i : i + 1, :] = d_ref[0, :, 128 * i : 128 * i + 128]
    for i in range(12):
        o_ref[36 + i : 37 + i, :] = s_ref[0, :, 128 * i : 128 * i + 128].astype(F32)
    for i in range(4):
        v = nb_ref[0, :, 128 * i : 128 * i + 128].astype(F32)
        for c in range(4):
            t_ref[4 * i + c : 4 * i + c + 1, :] = pltpu.roll(v, (128 - 32 * c) % 128, axis=1)
    o_ref[48:80, 0:NS] = t_ref[...].T[0:32, 0:NS]
    lane = lax.broadcasted_iota(jnp.int32, (1, NS), 1)
    o_ref[80:81, 0:NS] = ce_ref[0].astype(F32)
    o_ref[81:82, 0:NS] = jnp.where(lane < al_ref[0], ct_ref[0], 0).astype(F32)


def zperm():
    m = np.zeros((3, 128, 256), np.float32)
    for s in range(16):
        d, z = (1, s + 4) if s < 4 else ((0, s - 4) if s < 12 else (2, s - 12))
        for a in range(3):
            at = (s // 8) * 128 + (s % 8) * 12 + a * 4
            for c in range(3):
                m[d, z * 9 + a * 3 + c, at + c] = 1.0
            m[d, 72 + z * 3 + a, at + 3] = 1.0
    return m.reshape(384, 256)


def zrows_kernel(e_ref, g_ref, p_ref, o_ref, l_ref, lo_ref, hi_ref, t_ref):
    e = e_ref[0]
    lane = lax.broadcasted_iota(jnp.int32, (4, 128), 1)
    wide = lax.broadcasted_iota(jnp.int32, (LIST, 128), 1)
    lists = jnp.zeros((LIST, 128), F32)
    for d in range(3):
        at = lax.rem(e + (0, 3, 1)[d], 4)
        for j in range(16):
            r, off = divmod(72 * j, 128)
            v = g_ref[at, pl.ds(r, 4, stride=9), :]
            v = pltpu.roll(v, (128 - off) % 128, axis=1) if off else v
            if off + 72 > 128:
                n = g_ref[at, pl.ds(r + 1, 4, stride=9), :]
                n = pltpu.roll(n, 128 - off, axis=1)
                v = jnp.where(lane < 128 - off, v, n)
            r, off = divmod(24 * j, 128)
            k = g_ref[at, pl.ds(36 + r, 4, stride=3), :]
            k = pltpu.roll(k, (72 - off) % 128, axis=1)
            if off + 24 > 128:
                n = g_ref[at, pl.ds(37 + r, 4, stride=3), :]
                n = pltpu.roll(n, (72 - off) % 128, axis=1)
                k = jnp.where(lane < 72 + 128 - off, k, n)
            v = jnp.where(lane < 72, v, jnp.where(lane < 96, k, 0.0))
            t_ref[d, pl.ds(j, 4, stride=16), :] = v
        b = NS * (1, 0, 2)[d]
        v = g_ref[at, 48 : 48 + LIST, :]
        v = pltpu.roll(v, b, axis=1) if b else v
        lists = jnp.where((wide >= b) & (wide < b + NS), v, lists)
    rows = jnp.concatenate([t_ref[0], t_ref[1], t_ref[2]], axis=1)
    r = mm(jnp.concatenate(split(rows, 3), axis=0), p_ref[...])
    r = (r[0:64] + r[64:128]) + r[128:192]
    l_ref[...] = lists
    for h in range(2):
        v = r[:, 128 * h : 128 * h + 128]
        o_ref[h] = v
        lo_ref[32 * h : 32 * h + 32, :] = v[0:32]
        hi_ref[32 * h : 32 * h + 32, :] = v[32:64]
    lo_ref[64 : 64 + LIST, :] = lists
    hi_ref[64 : 64 + LIST, :] = lists


def yslab_kernel(o_ref, l_ref, m_ref, p_ref, la_ref, lo_ref, hi_ref):
    lane = lax.broadcasted_iota(jnp.int32, (LIST, 128), 1)
    first = jnp.where(lane < 48, l_ref[...], pltpu.roll(m_ref[64 : 64 + LIST, :], 48, axis=1))
    second = p_ref[64 : 64 + LIST, :]
    la_ref[0:LIST, :] = first
    la_ref[LIST : 2 * LIST, :] = second
    for out, base in ((lo_ref, 0), (hi_ref, 4)):
        for h in range(2):
            for k in range(4):
                at = 64 * h + 16 * k
                out[at : at + 8, :] = o_ref[h, pl.ds(base + k, 8, stride=8), :]
                out[at + 8 : at + 12, :] = m_ref[pl.ds(32 * h + base + k, 4, stride=8), :]
                out[at + 12 : at + 16, :] = p_ref[pl.ds(32 * h + base + k, 4, stride=8), :]
        out[128 : 128 + LIST, :] = first
        out[128 + LIST : 128 + 2 * LIST, :] = second


def weights_kernel(w2, wl, we, wot, ro, t2, tl, te, to, bo, be, bl, b2, rc):
    def three(w):
        h, l = split(w, 2)
        return jnp.concatenate([h, h, l], axis=1)

    pad = jnp.concatenate([w2[...], jnp.zeros((4, 64), F32)], axis=0)
    t2[...] = three(pad.T)
    tl[...] = three(wl[...].T)
    te[...] = three(we[...].T)
    to[...] = three(wot[...])
    bo[...] = three(wot[...].T)
    be[...] = three(we[...])
    bl[...] = three(wl[...])
    b2[...] = three(w2[4:12, :])
    eye = lax.broadcasted_iota(jnp.int32, (64, 64), 0) == lax.broadcasted_iota(
        jnp.int32, (64, 64), 1
    )
    rc[...] = jnp.sum(jnp.where(eye, jnp.broadcast_to(ro[...], (64, 64)), 0.0), axis=1, keepdims=True)


def poly(x, coefs):
    acc = jnp.full_like(x, coefs[-1])
    for c in coefs[-2::-1]:
        acc = acc * x + c
    return acc


SIN = [math.pi ** (2 * k + 1) * (-1) ** k / math.factorial(2 * k + 1) for k in range(7)]
COS = [math.pi ** (2 * k) * (-1) ** k / math.factorial(2 * k) for k in range(8)]
R3, R5, R15 = math.sqrt(3.0), math.sqrt(5.0), math.sqrt(15.0)
ORDER = (0, 1, 1, 1, 2, 2, 2, 2, 2)


def stack3(v):
    h, l = split(v, 2)
    return jnp.concatenate([h, l, h], axis=0)


def tree(parts):
    while len(parts) > 1:
        parts = [a + b for a, b in zip(parts[0::2], parts[1::2])] + parts[len(parts) & ~1 :]
    return parts[0]


def fold(v):
    return tree([v[:, 128 * i : 128 * i + 128] for i in range(TILES)])


def wide(v):
    return jnp.concatenate([v] * TILES, axis=1)


def div(v, k):
    return jnp.floor((v + 0.5) * (1.0 / k))


def cell_of(ce):
    cell = div(ce, 3)
    xy = div(cell, 8)
    x = div(xy, 8)
    return x, xy - 8.0 * x, cell - 8.0 * xy, ce - 3.0 * cell


def table_row(p, q):
    px = jnp.where(p < 4.0, p + 8.0, jnp.where(p < 12.0, p - 4.0, p))
    mid = q - 4.0 + 8.0 * jnp.where(p < 4.0, p + 8.0, jnp.where(p < 12.0, p - 4.0, p))
    return jnp.where(q < 4.0, 128.0 + 16.0 * q + px, jnp.where(q < 12.0, mid, 16.0 * q + px))


def place(x, y, z, atom):
    return (
        x + jnp.where(atom == 1.0, 0.75, 0.25),
        y + jnp.where(atom >= 1.0, 0.75, 0.25),
        z + jnp.where(atom == 2.0, 0.75, 0.25),
    )


def fperm():
    m = np.zeros((128, 128), np.float32)
    for z in range(8):
        for a in range(3):
            for c in range(3):
                m[z * 12 + a * 4 + c, z * 9 + a * 3 + c] = 1.0
    return m


def tiles(of):
    lane = lax.broadcasted_iota(jnp.int32, of, 1)
    row = lax.broadcasted_iota(jnp.int32, of, 0) if of[1] == 128 else lax.shift_right_logical(lane, 7)
    lane = lane & 127
    step = lax.shift_right_logical(row, 1)
    second = row & 1
    dy = jnp.where(step == 0, 0, jnp.where(step == 1, -1, 1))
    dx = jnp.where(second == 1, 1, jnp.where(lane < 48, 0, -1))
    at = jnp.where(lane < 48, lane, lane - 48)
    dz = lax.shift_right_logical(at, 4) - 1
    valid = (row < 6) & (lane < jnp.where(second == 1, 48, 96))
    return [v.astype(F32) for v in (dx, dy, dz)], valid, (row == 0) & (lane >= 16) & (lane < 32), lane


def main_kernel(
    o_ref, la_ref, xm_ref, xp_ref, ym_ref, yp_ref,
    t2, tl, te, to, bo, be, bl, b2, rc, fp_ref,
    en_ref, fo_ref,
    w_s, g_s, a_s, in_s, dw_s, sc_s, tb_s, ls_s, rk_s, acc_s, out_s, b_s, y_s, d_s,
):
    halves = []
    for h in range(2):
        v = jnp.concatenate(
            [
                o_ref[h], xm_ref[32 * h : 32 * h + 32, :], xp_ref[32 * h : 32 * h + 32, :],
                ym_ref[64 * h : 64 * h + 64, :], yp_ref[64 * h : 64 * h + 64, :],
            ],
            axis=0,
        )
        halves.append(v.T[0:96])
    tb_s[...] = jnp.concatenate(split(jnp.concatenate(halves, axis=0), 2), axis=1)

    places = [(la_ref, 0), (la_ref, LIST), (ym_ref, 128), (ym_ref, 128 + LIST), (yp_ref, 128), (yp_ref, 128 + LIST)]
    lst = jnp.concatenate([ref[at : at + LIST, :] for ref, at in places], axis=1)
    high = jnp.floor(lst[0:33] * (1.0 / 64.0))
    low = lst[0:33] - 64.0 * high
    (dx, dy, dz), valid, own, lane = tiles((8, 128))
    pad = jnp.zeros((2, 128), F32)
    ce = jnp.concatenate([ref[at + 32 : at + 33, :] for ref, at in places] + [pad], axis=0)
    ct = jnp.concatenate([ref[at + 33 : at + 34, :] for ref, at in places] + [pad], axis=0)
    cx, cy, cz, _ = cell_of(ce)
    flag = valid & (~own) & (ct > 0.0)
    for c, d in ((cx, dx), (cy, dy), (cz, dz)):
        v = c + 8.0 * d
        flag = flag & (v >= -2.0) & (v < 10.0)
    mine = jnp.where(own & (ct > 0.0), 1.0, 0.0)
    flag = jnp.where(flag, 1.0, 0.0)
    units = div(ct + (TILES - 1.0), TILES)
    tri = lax.broadcasted_iota(jnp.int32, (128, 128), 0) <= lax.broadcasted_iota(
        jnp.int32, (128, 128), 1
    )
    both = jnp.concatenate([units * flag, flag, units * mine, mine], axis=0)
    upto = mm(both.astype(BF16), jnp.where(tri, 1.0, 0.0).astype(BF16))
    total = jnp.broadcast_to(jnp.sum(both, axis=1, keepdims=True), (32, 128))
    row = lax.broadcasted_iota(jnp.int32, (8, 128), 0)

    def running(k):
        t = jnp.where(row >= 1, pltpu.roll(total[8 * k : 8 * k + 8], 1, axis=0), 0.0)
        for by in (1, 2, 4):
            t = t + jnp.where(row >= by, pltpu.roll(t, by, axis=0), 0.0)
        return upto[8 * k : 8 * k + 8] + t

    def start(k):
        o = upto[8 * k + 16 : 8 * k + 24] - both[8 * k + 16 : 8 * k + 24]
        g = running(k) - both[8 * k : 8 * k + 8] + total[8 * k + 16 : 8 * k + 17]
        return jnp.where(mine > 0.0, o, g)

    needed = jnp.sum(both[0:8]) + jnp.sum(both[16:24])
    listed = jnp.sum(both[8:16]) + jnp.sum(both[24:32])
    fits = needed <= 128.0
    index = start(1)
    block_of = div(index, FULL)
    rank = jnp.where(fits, start(0), 128.0 * block_of + 3.0 * (index - FULL * block_of))
    used = (mine + flag) > 0.0
    rk_s[0:8, :] = jnp.where(used, rank, 1e6)
    rk_s[8:16, :] = jnp.where(used, rank + jnp.where(fits, units, 3.0), 0.0)
    blocks = jnp.where(fits, 1, lax.div(listed.astype(jnp.int32) + (FULL - 1), FULL))
    rank = jnp.where(used, rank, 0.0)
    at = jnp.concatenate([rank[t : t + 1] for t in range(6)], axis=1)
    (dx, dy, dz), _, _, _ = tiles((1, 768))
    ls_s[...] = jnp.concatenate(
        [
            high[0:32], low[0:32], high[32:33], low[32:33], lst[33:34],
            dx + 1.0, dy + 1.0, dz + 1.0, jnp.floor(at * (1.0 / 64.0)), at - 64.0 * jnp.floor(at * (1.0 / 64.0)),
            jnp.zeros((8, 768), F32),
        ],
        axis=0,
    ).astype(BF16)
    acc_s[...] = jnp.zeros((64, 128), F32)
    sc_s[...] = jnp.zeros((8, PAIRS + 128), F32)
    in_s[12:16, :] = jnp.zeros((4, PAIRS), F32)

    def block(b, carry):
        want = (lax.broadcasted_iota(jnp.int32, (128, 128), 0) + 128 * b).astype(F32)
        chosen = jnp.concatenate(
            [
                jnp.where(
                    (want >= rk_s[t : t + 1, :]) & (want < rk_s[8 + t : 9 + t, :]), 1.0, 0.0
                ).astype(BF16)
                for t in range(6)
            ],
            axis=1,
        )
        u = mm(ls_s[...], chosen, ((1,), (1,)))
        key = 64.0 * u[70:71] + u[71:72]
        part = (lax.broadcasted_iota(jnp.int32, (1, 128), 1) + 128 * b).astype(F32) - key
        keys = jnp.broadcast_to(key, (128, 128))
        comb = jnp.where(keys == keys.T, 1.0, 0.0).astype(BF16)
        comb = jnp.concatenate([comb, comb], axis=0)

        def slots_sum(v):
            return mm(jnp.concatenate(split(v, 2), axis=1), comb)

        def slots(at):
            def pick_slot(t):
                v = [u[at + t + k : at + t + k + 1] for k in (0, TILES, 2 * TILES) if t + k < 32]
                late = v[2] if len(v) > 2 else jnp.zeros((1, 128), F32)
                return jnp.where(part < 0.5, v[0], jnp.where(part < 1.5, v[1], late))

            return jnp.concatenate([pick_slot(t) for t in range(TILES)], axis=1)

        nb = 64.0 * slots(0) + slots(32)
        ce = 64.0 * u[64:65] + u[65:66]
        count = u[66:67]
        shift = [8.0 * (u[67 + k : 68 + k] - 1.0) for k in range(3)]
        cx, cy, cz, ca = cell_of(ce)
        cx, cy, cz = cx + shift[0], cy + shift[1], cz + shift[2]
        pq = div(nb, 36)
        r = nb - 36.0 * pq
        p = div(pq, 12)
        q = pq - 12.0 * p
        s = div(r, 3)
        a = r - 3.0 * s
        p = p + wide(shift[0] - 2.0)
        q = q + wide(shift[1] - 2.0)
        s = s + wide(shift[2] - 2.0)
        lane = lax.broadcasted_iota(jnp.int32, (1, PAIRS), 1)
        alive = lax.shift_right_logical(lane, 7).astype(F32) < wide(count - TILES * part)
        live = jnp.where(alive, 1.0, 0.0)
        second = place(p, q, s, a)
        centre = place(cx, cy, cz, ca)
        geo = [second[k] - wide(centre[k]) for k in range(3)]
        rows = jnp.concatenate([table_row(p + 4.0, q + 4.0), table_row(cx + 4.0, cy + 4.0)], axis=1)
        rsel = jnp.concatenate([3.0 * (s + 4.0) + a, 3.0 * (cz + 4.0) + ca], axis=1)
        at = lax.broadcasted_iota(jnp.int32, (256, PAIRS + 128), 0).astype(F32).astype(BF16)
        hot = jnp.where(at == jnp.broadcast_to(rows.astype(BF16), at.shape), jnp.ones_like(at), jnp.zeros_like(at))

        got = mm(tb_s[...], jnp.concatenate([hot, hot], axis=0))
        half = lax.shift_right_logical(
            lax.broadcasted_iota(jnp.int32, (8, PAIRS + 128), 0), 2
        ).astype(F32)
        pick = jnp.zeros((8, PAIRS + 128), F32)
        for k in range(24):
            pick = jnp.where(half + 2.0 * k == rsel, got[8 * k : 8 * k + 8], pick)
        pick = pick[0:4] + pick[4:8]
        first = wide(pick[:, PAIRS:])
        second = pick[:, 0:PAIRS]
        rx = [
            jnp.where(alive, (geo[k] + (second[k : k + 1] - first[k : k + 1])) * CELL, 1.0)
            for k in range(3)
        ]
        d2 = rx[0] * rx[0] + rx[1] * rx[1] + rx[2] * rx[2]
        inv = lax.rsqrt(d2)
        inv = inv * (1.5 - 0.5 * d2 * inv * inv)
        dist = d2 * inv
        ux, uy, uz = [v * inv for v in rx]
        x = dist * (1.0 / CUT)
        inside = x < 1.0
        x = jnp.minimum(x, 1.0)
        x2 = x * x
        x3 = x2 * x
        x5 = x3 * x2
        x6 = x3 * x3
        env = jnp.where(inside, 1.0 + x6 * (-28.0 + x * (48.0 - 21.0 * x)), 0.0)
        denv_dd = jnp.where(inside, (-168.0 / CUT) * x5 * (1.0 - x) * (1.0 - x), 0.0)
        ev = env * live

        n = (lax.broadcasted_iota(jnp.int32, (8, PAIRS), 0) + 1).astype(F32)
        t = n * x
        k = jnp.floor(t + 0.5)
        f = t - k
        sign = 1.0 - 2.0 * (k - 2.0 * jnp.floor(k * 0.5))
        f2 = f * f
        sn = sign * f * poly(f2, SIN)
        cs = sign * poly(f2, COS)
        c0 = math.sqrt(2.0 / CUT)
        sd = sn * (c0 * inv)
        basis = sd * env
        dbasis = (n * cs) * ((c0 * math.pi / CUT) * inv * env) + sd * (denv_dd - env * inv)
        k1, k2 = first[3:4], second[3:4]
        in_s[0:1, :] = jnp.where(k1 == 0.0, 1.0, 0.0)
        in_s[1:2, :] = jnp.where(k1 == 1.0, 1.0, 0.0)
        in_s[2:3, :] = jnp.where(k2 == 0.0, 1.0, 0.0)
        in_s[3:4, :] = jnp.where(k2 == 1.0, 1.0, 0.0)
        in_s[4:12, :] = basis

        def silu(v):
            sg = 0.5 + 0.5 * jnp.tanh(0.5 * v)
            return v * sg, sg * (1.0 + v * (1.0 - sg))

        h, dh_ = silu(mm(t2[...], stack3(in_s[...])))
        z, dz_ = silu(mm(tl[...], stack3(h)))
        zs = stack3(z)
        e = mm(te[...], zs)
        w_s[...] = e * ev

        ys = [
            None, R3 * ux, R3 * uy, R3 * uz, R15 * ux * uy, R15 * uy * uz,
            (0.5 * R5) * (3.0 * uz * uz - 1.0), R15 * ux * uz, (0.5 * R15) * (ux * ux - uy * uy),
        ]
        for m in range(1, 9):
            y_s[m : m + 1, :] = ys[m]

        def each_group(make):
            def run(c, carry):
                at = slice(8 * c, 8 * c + 8)
                for l, first_m, last_m in ((0, 0, 1), (1, 1, 4), (2, 4, 9)):
                    v = [make(at, c, l, i) for i in range(TILES)]
                    for m in range(first_m, last_m):
                        b_s[m, at, :] = 0.2 * tree(
                            [
                                v[i] if m == 0 else v[i] * y_s[m : m + 1, 128 * i : 128 * i + 128]
                                for i in range(TILES)
                            ]
                        )
                return carry

            for c in range(8):
                run(c, 0)
            return slots_sum(b_s[...].reshape(576, 128)).reshape(9, 64, 128)

        a_s[...] = each_group(lambda at, c, l, i: w_s[at, 128 * i : 128 * i + 128])

        def weigh(i, carry):
            at = slice(128 * i, 128 * i + 128)
            yt = [None] + [jnp.broadcast_to(y_s[m : m + 1, at], (8, 128)) for m in range(1, 9)]
            for c in range(8):
                rows = slice(8 * c, 8 * c + 8)
                sums = [None, None, None]
                for m in range(9):
                    term = a_s[m, rows, :] if m == 0 else yt[m] * a_s[m, rows, :]
                    l = ORDER[m]
                    sums[l] = term if sums[l] is None else sums[l] + term
                for l in range(3):
                    g_s[64 * l + 8 * c : 64 * l + 8 * c + 8, at] = sums[l] * w_s[rows, at]
            return carry

        for i in range(TILES):
            weigh(i, 0)
        joined = jnp.concatenate([z, g_s[...]], axis=0)
        y, dy_ = silu(mm(to[...], stack3(joined)))
        ro = rc[...]
        raw = jnp.sum(ro * y, axis=0, keepdims=True)

        @pl.when(b == 0)
        def _():
            en = jnp.concatenate(split(fold(raw * ev), 3) + [jnp.zeros((5, 128), BF16)], axis=0)
            en = jnp.sum(mm(en, chosen[:, 0:128]), axis=0, keepdims=True)
            en_ref[...] = en[:, NS : 2 * NS].reshape(1, 1, NS)

        denv = live * raw
        dj = mm(bo[...], stack3((ro * ev) * dy_))
        g_s[...] = dj[64:256]

        def grown(at, c, l, i):
            tile = slice(128 * i, 128 * i + 128)
            return g_s[64 * l + 8 * c : 64 * l + 8 * c + 8, tile] * w_s[at, tile]

        b_s[...] = each_group(grown)

        def back(i, carry):
            at = slice(128 * i, 128 * i + 128)
            yt = [None] + [jnp.broadcast_to(y_s[m : m + 1, at], (8, 128)) for m in range(1, 9)]
            acc = [None] * 9
            for c in range(8):
                rows = slice(8 * c, 8 * c + 8)
                w = w_s[rows, at]
                g = [g_s[64 * l + 8 * c : 64 * l + 8 * c + 8, at] for l in range(3)]
                dw = None
                for m in range(9):
                    t = g[ORDER[m]] * a_s[m, rows, :] + b_s[m, rows, :]
                    v = t if m == 0 else yt[m] * t
                    dw = v if dw is None else dw + v
                    if m:
                        acc[m] = w * t if acc[m] is None else acc[m] + w * t
                dw_s[rows, at] = dw
            for m in range(1, 9):
                d_s[m : m + 1, at] = jnp.sum(acc[m], axis=0, keepdims=True)
            return carry

        for i in range(TILES):
            back(i, 0)
        dw = dw_s[...]
        denv = denv + live * jnp.sum(dw * e, axis=0, keepdims=True)
        dz = dj[0:64] + mm(be[...], stack3(dw * ev))
        dh = mm(bl[...], stack3(dz * dz_))
        db = mm(b2[...], stack3(dh * dh_))
        dd = denv * denv_dd + jnp.sum(db * dbasis, axis=0, keepdims=True)
        dy = [None] + [d_s[m : m + 1, :] for m in range(1, 9)]
        du0 = R3 * dy[1] + R15 * (uy * dy[4] + uz * dy[7] + ux * dy[8])
        du1 = R3 * dy[2] + R15 * (ux * dy[4] + uz * dy[5] - uy * dy[8])
        du2 = R3 * dy[3] + R15 * (uy * dy[5] + ux * dy[7]) + (3.0 * R5) * uz * dy[6]
        along = ux * du0 + uy * du1 + uz * du2
        dd = dd - along * inv
        grad = [du0 * inv + ux * dd, du1 * inv + uy * dd, du2 * inv + uz * dd]
        for k in range(3):
            mine = fold(grad[k])
            for row in (k, k + 4):
                sc_s[row : row + 1, 0:PAIRS] = -grad[k]
                sc_s[row : row + 1, PAIRS:] = mine
        gv = sc_s[...]
        m = jnp.concatenate(
            [jnp.where(half + (12.0 + 2.0 * k) == rsel, gv, 0.0) for k in range(12)]
            + [jnp.zeros((32, PAIRS + 128), F32)],
            axis=0,
        )
        mh, ml = split(m, 2)
        nt = ((1,), (1,))
        own = hot[0:64]
        acc_s[...] += mm(jnp.concatenate([own, own], axis=1), jnp.concatenate([mh, ml], axis=1), nt)
        return carry

    lax.fori_loop(0, blocks, block, 0)

    r = mm(jnp.concatenate(split(acc_s[...], 3), axis=0), fp_ref[...])
    out_s[...] = (r[0:64] + r[64:128]) + r[128:192]
    lane = lax.broadcasted_iota(jnp.int32, (4, 128), 1)
    for k in range(9):
        v = jnp.zeros((4, 128), F32)
        for j in range(128 * k // 72, (128 * k + 127) // 72 + 1):
            off = 72 * j - 128 * k
            part = pltpu.roll(out_s[pl.ds(j, 4, stride=16), :], off % 128, axis=1)
            v = v + jnp.where((lane >= off) & (lane < off + 72), part, 0.0)
        for g in range(4):
            fo_ref[0, :, 128 * (9 * g + k) : 128 * (9 * g + k) + 128] = v[g : g + 1]


def sds(shape, dtype=F32):
    return jax.ShapeDtypeStruct(shape, dtype)


def hop(v, axis, by):
    n = lax.axis_size(axis)
    return lax.ppermute(v, axis, [(i, (i + by) % n) for i in range(n)])


def local(
    displacement, species, centres, neighbours, neighbour_count, live_centres,
    w_two, w_lat, w_env, w_out, readout,
):
    e = lax.axis_index("gz").astype(jnp.int32).reshape(1)
    flat = call(
        pack_kernel,
        sds((48 + LIST, 128)),
        [
            (pltpu.with_memory_space_constraint(v, pltpu.HBM), HB)
            for v in (displacement, species, neighbours, centres, neighbour_count)
        ]
        + [(live_centres.reshape(1), SM)],
        "pack",
        [
            pltpu.VMEM((128, 128), F32), pltpu.VMEM((1, 1, 4608), F32),
            pltpu.VMEM((1, 1, 1536), jnp.int32), pltpu.VMEM((1, 1, 512), jnp.int32),
            pltpu.VMEM((1, 1, NS), jnp.int32), pltpu.VMEM((1, 1, NS), jnp.int32),
            pltpu.SemaphoreType.DMA((5,)),
        ],
    )
    column = lax.all_gather(flat, "gz")
    slab = sds((64 + LIST, 128))
    own, lists, lo, hi = call(
        zrows_kernel,
        (sds((2, 64, 128)), sds((LIST, 128)), slab, slab),
        [(e, SM), (column, VM), (jnp.asarray(zperm(), BF16), VM)],
        "zrows",
        [pltpu.VMEM((3, 64, 128), F32)],
    )
    xm, xp = hop(hi, "gx", 1), hop(lo, "gx", -1)
    ws = call(
        weights_kernel,
        (
            sds((64, 48), BF16), sds((64, 192), BF16), sds((64, 192), BF16), sds((64, 768), BF16),
            sds((256, 192), BF16), sds((64, 192), BF16), sds((64, 192), BF16), sds((8, 192), BF16),
            sds((64, 1)),
        ),
        [(v, VM) for v in (w_two, w_lat, w_env, w_out.T, readout.reshape(1, 64))],
        "weights",
    )
    slab = sds((128 + 2 * LIST, 128))
    lists, lo, hi = call(
        yslab_kernel,
        (sds((2 * LIST, 128)), slab, slab),
        [(v, VM) for v in (own, lists, xm, xp)],
        "yslab",
    )
    ym, yp = hop(hi, "gy", 1), hop(lo, "gy", -1)
    return call(
        main_kernel,
        (sds((1, 1, NS)), sds((1, 1, 4608))),
        [(v, VM) for v in (own, lists, xm, xp, ym, yp, *ws, jnp.asarray(fperm(), BF16))],
        "pairs",
        [
            pltpu.VMEM((64, PAIRS), F32),
            pltpu.VMEM((192, PAIRS), F32), pltpu.VMEM((9, 64, 128), F32),
            pltpu.VMEM((16, PAIRS), F32), pltpu.VMEM((64, PAIRS), F32),
            pltpu.VMEM((8, PAIRS + 128), F32), pltpu.VMEM((192, 512), BF16),
            pltpu.VMEM((80, 768), BF16), pltpu.VMEM((16, 128), F32),
            pltpu.VMEM((64, 128), F32), pltpu.VMEM((64, 128), F32),
            pltpu.VMEM((9, 64, 128), F32), pltpu.VMEM((16, PAIRS), F32), pltpu.VMEM((16, PAIRS), F32),
        ],
        mib=24,
    )


def solution(mesh):
    cut = P("gx", "gy", "gz")
    return jax.shard_map(
        local,
        mesh=mesh,
        in_specs=(cut,) * 6 + (P(),) * 5,
        out_specs=(cut, cut),
        check_vma=False,
    )
```
